128 devices in a mesh: dp: 32 (over z, y, core), tensor: 4 (over x).
Axes of the slice: x: 4, y: 4, z: 4, core: 2. Of those that a mesh axis runs over, the one named last changes fastest.
Arguments:
- tokens: bfloat16 [12288, 2880], P('dp', 'tensor'), may hold values from -6 to 6
- out_grad: bfloat16 [12288, 2880], P('dp', 'tensor'), may hold values from -6 to 6
- route_probs: bfloat16 [12288, 4], P('dp'), may hold values from 0.099609375 to 1
- expert_ids: int32 [12288, 4], P('dp'), may hold values from 0 to 127, all different within a row; in each aligned block of 384 rows (0 to 383, 384 to 767, ...) at most 18 rows name the same one
- placement_map: int32 [128], replicated, may hold values from 0 to 127, each once
- w_gate: bfloat16 [32, 2880, 2880], P('dp', None, 'tensor'), may hold values from -0.109375 to 0.109375
- w_up: bfloat16 [32, 2880, 2880], P('dp', None, 'tensor'), may hold values from -0.109375 to 0.109375
- w_down: bfloat16 [32, 2880, 2880], P('dp', 'tensor'), may hold values from -0.109375 to 0.109375
Outputs:
- input_grad: bfloat16 [12288, 2880], P('dp', 'tensor')
- gate_grad: bfloat16 [32, 2880, 2880], P('dp', None, 'tensor')
- up_grad: bfloat16 [32, 2880, 2880], P('dp', None, 'tensor')
- down_grad: bfloat16 [32, 2880, 2880], P('dp', 'tensor')
- prob_grad: bfloat16 [12288, 4], P('dp')
The draws below stay inside these ranges and needn't reach their ends.
Inputs may be any that keep to these rules, and one draw needn't show every extreme that they name: `expert_ids`: each row names 4 different experts. In the rows of one index of dp no expert is named by more than 18 rows, a bound that some block reaches. `placement_map`: A permutation: every value is taken by exactly one expert.
All inputs are finite; a program needn't handle non-finite values.
Results may differ from the reference program's by a relative error of at most 0.011.
Values may be sent and summed in bfloat16 or wider, within the bound.
A program may use at most 128 MiB of HBM per device.

```python
import math
import jax
import jax.numpy as jnp
import numpy as np
from jax import lax

D = 2880
FF = 2880
TOP = 4
EXP_OWN = 4
EXPERTS = 128
TOK_DEV = 384
TOKENS = 12288
CAP = 18
N_DP = 32
N_TENSOR = 4


def steps_of(rng, dims, split, least, high):
    loudness, own = 1.0, jax.random.fold_in(rng, 6)
    for dim, blocks in split:
        draws = jnp.exp(jax.random.uniform(jax.random.fold_in(own, dim), (blocks,), jnp.float32, least / len(split), high / len(split)))
        loudness = loudness * jnp.repeat(draws, dims[dim] // blocks).reshape([-1 if axis == dim else 1 for axis in range(len(dims))])
    return loudness


def deal_out(own_key, own, number, rows, count, top, limit, slope):
    sequence = jax.random.permutation(own_key, count)
    packed, ordinary = shares(count, rows * top, limit, slope, True), shares(count, rows * top, limit, slope, False)
    places = jnp.arange(count)

    def named(tallies, offset_by):
        used = int((tallies > 0).sum())
        fixed = max(1, used // 4)
        passed = fixed + (places - fixed + offset_by * (used - fixed)) % max(1, count - fixed)
        return jnp.zeros((count,), jnp.int32).at[sequence[jnp.where(places < fixed, places, passed)]].set(jnp.asarray(tallies, jnp.int32))

    tallies = jnp.where(number % 4 == 0, named(packed, number // 4), named(ordinary, number - number // 4 - 1))
    mixed = jax.random.permutation(jax.random.fold_in(own, 3), count)
    donor, receiver = mixed[0:count // 2 * 2:2], mixed[1:count // 2 * 2:2]
    slack = jnp.minimum(tallies[donor] - 1, limit - tallies[receiver]) // 2
    slack = jnp.where((donor == sequence[0]) | (receiver == sequence[0]) | (tallies[receiver] == 0), 0, jnp.maximum(slack, 0))
    passed = jax.random.randint(jax.random.fold_in(own, 4), (count // 2,), 0, 1 << 20) % (slack + 1)
    tallies = tallies.at[donor].add(-passed).at[receiver].add(passed)
    members = jnp.searchsorted(jnp.cumsum(tallies), jnp.arange(rows * top), side="right").astype(jnp.int32)
    table = members.reshape(top, rows).T
    table = table[jax.random.permutation(jax.random.fold_in(own, 1), rows)]
    offset_by = jax.random.randint(jax.random.fold_in(own, 2), (rows, 1), 0, top)
    return jnp.take_along_axis(table, (jnp.arange(top)[None, :] + offset_by) % top, axis=1)


def shares(amount, total, reach, slope, full):
    loads = [(1 << 20) // math.isqrt(rank ** slope) + 1 for rank in range(1, amount + 1)]
    largest = reach if full else min(reach, max(-(-total // amount), total * loads[0] // sum(loads)))
    least = 1 if total - largest >= amount - 1 else 0
    counts, surplus = [largest] + [least] * (amount - 1), total - largest - least * (amount - 1)
    while surplus > 0:
        candidates = [i for i in range(1, amount) if counts[i] < largest] or [i for i in range(1, amount) if counts[i] < reach]
        mass, left = sum([loads[i] for i in candidates]), surplus
        for i in candidates:
            extra = min(reach - counts[i], max(1, left * loads[i] // mass), surplus)
            counts[i] = counts[i] + extra
            surplus = surplus - extra
    return np.array(counts)


def scatter_about(own_key, extent, deviation, most, shards=(), kind=jnp.bfloat16):
    array = deviation * jax.random.normal(own_key, extent, jnp.float32)
    if shards:
        array = array * steps_of(own_key, extent, shards, -0.22, 0.18)
    return jnp.clip(array, -most, most).astype(kind)


def setup_inputs(seed: int = 0) -> dict:
    splits = jax.random.split(jax.random.key(seed), 9)
    tokens = scatter_about(splits[0], (TOKENS, D), 1.0, 6.0, ((0, 32), (1, 4)))
    out_grad = scatter_about(splits[1], (TOKENS, D), 1.0, 6.0, ((0, 32), (1, 4)))
    route_probs = jnp.clip(0.099609375 + 0.9003906 * jax.random.uniform(splits[2], (TOKENS, TOP), jnp.float32) ** steps_of(splits[2], (TOKENS, TOP), ((0, 32),), -0.2, 0.2), 0.099609375, 1.0).astype(jnp.bfloat16)
    expert_ids_keys = jax.random.split(jax.random.fold_in(splits[3], 1), TOKENS // TOK_DEV)
    expert_ids_turns = jax.random.permutation(jax.random.fold_in(splits[3], 3), TOKENS // TOK_DEV)
    expert_ids = jax.vmap(lambda own, number: deal_out(jax.random.fold_in(splits[3], 2), own, number, TOK_DEV, EXPERTS, TOP, CAP, 2))(expert_ids_keys, expert_ids_turns).reshape((TOKENS, TOP))
    placement_map = jax.random.permutation(splits[4], EXPERTS).astype(jnp.int32)
    w_gate = scatter_about(splits[5], (N_DP, D, FF), D ** -0.5, 0.109375, ((0, 32), (2, 4)))
    w_up = scatter_about(splits[6], (N_DP, D, FF), D ** -0.5, 0.109375, ((0, 32), (2, 4)))
    w_down = scatter_about(splits[7], (N_DP, FF, D), FF ** -0.5, 0.109375, ((0, 32), (1, 4)))
    return {"tokens": tokens, "out_grad": out_grad, "route_probs": route_probs, "expert_ids": expert_ids, "placement_map": placement_map, "w_gate": w_gate, "w_up": w_up, "w_down": w_down}


SWISH_SLOPE = 1.702


def wave_layout(expert_ids, placement_map):
    code_value = placement_map[expert_ids].reshape(N_DP, TOK_DEV * TOP)
    in_wave = code_value % EXP_OWN == 0
    owner_of = code_value // EXP_OWN
    owner_range = jnp.arange(N_DP, dtype=jnp.int32)
    chosen = ((owner_of[:, :, None] == owner_range[None, None, :]) & in_wave[:, :, None]).astype(jnp.int32)
    before = jnp.cumsum(chosen, axis=1) - chosen
    slot_index = jnp.sum(before * chosen, axis=2).astype(jnp.int32)
    position = owner_range[:, None] * CAP + slot_index
    return in_wave, owner_of, position


def reference(tokens, out_grad, route_probs, expert_ids, placement_map, w_gate, w_up, w_down):
    in_wave, owner_of, position = wave_layout(expert_ids, placement_map)
    route_ids = jnp.arange(TOKENS * TOP, dtype=jnp.int32).reshape(N_DP, TOK_DEV * TOP)
    owner_row = jnp.where(in_wave, owner_of, N_DP).astype(jnp.int32)
    slot_route = jnp.full((N_DP, N_DP * CAP), -1, jnp.int32).at[owner_row, position].set(route_ids, mode="drop")
    flat_probs = route_probs.reshape(-1)
    zero_half = jnp.zeros((), jnp.bfloat16)
    block_width = FF // N_TENSOR

    def expert_backward(operands):
        gate_w, up_w, down_w, routes = operands
        row_valid = routes >= 0
        safe_route = jnp.where(row_valid, routes, 0).astype(jnp.int32)
        token_index = (safe_route // TOP).astype(jnp.int32)
        rows_x = jnp.where(row_valid[:, None], tokens[token_index], zero_half)
        rows_d = jnp.where(row_valid[:, None], out_grad[token_index], zero_half)
        prob_column = jnp.where(row_valid, flat_probs[safe_route], zero_half).astype(jnp.float32)[:, None]
        gate_pre = jnp.dot(rows_x, gate_w, preferred_element_type=jnp.float32)
        up_pre = jnp.dot(rows_x, up_w, preferred_element_type=jnp.float32)
        sig_gate = jax.nn.sigmoid(SWISH_SLOPE * gate_pre)
        active = (gate_pre * sig_gate * (up_pre + 1.0)).astype(jnp.bfloat16)
        down_back = jnp.dot(rows_d, down_w.T, preferred_element_type=jnp.float32)
        prob_sum = jnp.sum(active.astype(jnp.float32) * down_back, axis=1)
        delta_act = prob_column * down_back
        grad_gate_pre = (delta_act * (up_pre + 1.0) * (sig_gate + SWISH_SLOPE * gate_pre * sig_gate * (1.0 - sig_gate))).astype(jnp.bfloat16)
        grad_up_pre = (delta_act * gate_pre * sig_gate).astype(jnp.bfloat16)
        scaled_grad = (prob_column * rows_d.astype(jnp.float32)).astype(jnp.bfloat16)
        down_grad = jnp.dot(active.T, scaled_grad, preferred_element_type=jnp.float32).astype(jnp.bfloat16)
        gate_grad = jnp.dot(rows_x.T, grad_gate_pre, preferred_element_type=jnp.float32).astype(jnp.bfloat16)
        up_grad = jnp.dot(rows_x.T, grad_up_pre, preferred_element_type=jnp.float32).astype(jnp.bfloat16)
        input_total = jnp.zeros((routes.shape[0], D), jnp.float32)
        for block in range(N_TENSOR):
            lower = block * block_width
            upper = lower + block_width
            partial_rows = (jnp.dot(grad_gate_pre[:, lower:upper], gate_w[:, lower:upper].T, preferred_element_type=jnp.float32)
                            + jnp.dot(grad_up_pre[:, lower:upper], up_w[:, lower:upper].T, preferred_element_type=jnp.float32))
            input_total = input_total + partial_rows.astype(jnp.bfloat16).astype(jnp.float32)
        input_rows = input_total.astype(jnp.bfloat16)
        return gate_grad, up_grad, down_grad, input_rows, prob_sum.astype(jnp.bfloat16)

    gate_grad, up_grad, down_grad, back_rows, back_prob = lax.map(expert_backward, (w_gate, w_up, w_down, slot_route))
    flat_index = (jnp.where(in_wave, owner_of, 0) * (N_DP * CAP) + jnp.where(in_wave, position, 0)).reshape(-1).astype(jnp.int32)
    wave_flat = in_wave.reshape(-1)
    route_rows = jnp.where(wave_flat[:, None], back_rows.reshape(N_DP * N_DP * CAP, D)[flat_index], zero_half)
    input_grad = jnp.sum(route_rows.reshape(TOKENS, TOP, D).astype(jnp.float32), axis=1).astype(jnp.bfloat16)
    prob_grad = jnp.where(wave_flat, back_prob.reshape(-1)[flat_index], zero_half).reshape(TOKENS, TOP)
    return input_grad, gate_grad, up_grad, down_grad, prob_grad
```

```python
import functools

import jax
import jax.numpy as jnp
import numpy as np
from jax import lax
from jax.experimental import pallas as pl
from jax.experimental.pallas import tpu as pltpu
from jax.sharding import PartitionSpec as P

SLOPE = 1.702
MESH = pl.DeviceIdType.MESH
NDP, NT = 32, 4
CAP = 18
TOK, F, FP = 384, 720, 768
SB, DOFF = 40, 20
RB = 24
PL = 8
G = 4
GR = PL * CAP
SRC_ORDER = (0, 1, 3, 2)
DST_ORDER = (0, 3, 1, 2)
LANES = (((1,), (1,)), ((), ()))
F32, BF16 = jnp.float32, jnp.bfloat16


def dot(a, b):
    return jnp.dot(a, b, preferred_element_type=F32)


def dot_lanes(a, b):
    return lax.dot_general(a, b, LANES, preferred_element_type=F32)


def iota(shape, dim):
    return lax.broadcasted_iota(jnp.int32, shape, dim)


def owner_table(pcol):
    return jnp.where(pcol == 4 * iota((128, 128), 1), 1.0, 0.0).astype(BF16)


def route_ranks(ids, table):
    hit = jnp.zeros((TOK, 128), F32)
    for k in range(4):
        hit += jnp.where(ids[:, k : k + 1] == iota((TOK, 128), 1), 1.0, 0.0)
    member = dot(hit.astype(BF16), table)
    lower = jnp.where(iota((TOK, TOK), 0) > iota((TOK, TOK), 1), 1.0, 0.0).astype(BF16)
    rank = dot(lower, member.astype(BF16))
    return jnp.where(member > 0.5, rank, -1.0).astype(BF16)


def comm_kernel(
    ids_ref, pcol_ref, probs_ref, tok_ref, og_ref, c40_ref, cx_ref, cd_ref, rx_ref, wg_hbm, wu_hbm, wd_hbm,
    x_out, d_out, dg_out, du_out, pa_out, back_out,
    send, recv, xb, db, wg, wu, wd, wdq, acc_g, acc_u, acc_d, dg, du, pa, prob, dxs, far_in, left_in, right_in, ret, ret_in,
    w_sem, a2a_s, a2a_r, gat_s, gat_r, far_s, far_r, out_s, left_r, right_r, ret_s, ret_r, o_sem,
):
    me = lax.axis_index("dp")
    t = lax.axis_index("tensor")
    z = me // PL
    right, left, far = (t + 1) % NT, (t + 3) % NT, (t + 2) % NT

    barrier = pltpu.get_barrier_semaphore()

    def greet(d, c):
        @pl.when(d != me)
        def _():
            pl.semaphore_signal(barrier, inc=1, device_id=(d, t), device_id_type=MESH)

        return c

    lax.fori_loop(0, NDP, greet, 0)
    for nb in (left, right):
        pl.semaphore_signal(barrier, inc=1, device_id=(me, nb), device_id_type=MESH)

    weights = [
        pltpu.make_async_copy(src, dst, w_sem.at[i])
        for i, (src, dst) in enumerate(((wg_hbm, wg), (wu_hbm, wu), (wd_hbm, wd)))
    ]
    for w in weights:
        w.start()

    ids = ids_ref[...]
    table = owner_table(pcol_ref[...])
    probs = probs_ref[...].astype(F32)
    ranks = route_ranks(ids, table)
    pw = jnp.zeros((TOK, 128), F32)
    for k in range(4):
        pw += jnp.where(ids[:, k : k + 1] == iota((TOK, 128), 1), probs[:, k : k + 1], 0.0)
    owner_p = dot(pw.astype(BF16), table).astype(BF16)

    def plane(order, i):
        return (z + order[i]) % G

    def build(zd):
        block, jx, jd = c40_ref[:, 0:1], c40_ref[:, 1:2], c40_ref[:, 2:3]
        mine = iota((PL * SB, 128), 1) == block + zd * PL
        slots = dot_lanes(jnp.where(mine, 1.0, 0.0).astype(BF16), ranks)
        hot_x = jnp.where(slots == jx.astype(F32), 1.0, 0.0).astype(BF16)
        hot_d = jnp.where(slots == jd.astype(F32), 1.0, 0.0).astype(BF16)
        rows = dot(hot_x, tok_ref[...]) + dot(hot_d, og_ref[...])
        p = jnp.sum(jnp.where(mine, dot(hot_x, owner_p), 0.0), axis=1, keepdims=True)
        for j in range(PL):
            part = slice(j * SB, (j + 1) * SB)
            send[zd * PL + j, :, 0:F] = rows[part].astype(BF16)
            send[zd * PL + j, :, F:FP] = jnp.broadcast_to(p[part], (SB, FP - F)).astype(BF16)

    def a2a(o):
        return pltpu.make_async_remote_copy(
            src_ref=send.at[o], dst_ref=recv.at[me], send_sem=a2a_s.at[o], recv_sem=a2a_r.at[me],
            device_id=(o, t), device_id_type=MESH)

    def a2a_in(s):
        return pltpu.make_async_remote_copy(
            src_ref=send.at[s], dst_ref=recv.at[s], send_sem=a2a_s.at[s], recv_sem=a2a_r.at[s],
            device_id=(s, t), device_id_type=MESH)

    def others(first, act):
        def body(j, c):
            o = first + j

            @pl.when(o != me)
            def _():
                act(o)

            return c

        lax.fori_loop(0, PL, body, 0)

    for i in range(G):
        zd = plane(DST_ORDER, i)
        build(zd)
        if i == 0:
            pl.semaphore_wait(barrier, NDP - 1 + 2)
            recv[me] = send[me]
        others(zd * PL, lambda o: a2a(o).start())

    for w in weights:
        w.wait()

    def quarter_rows(r, c):
        rows = pl.ds(pl.multiple_of(r * 144, 16), 144)
        for q in range(NT):
            wdq[q, rows, 0:F] = wd[rows, q * F : (q + 1) * F]
        return c

    lax.fori_loop(0, F // 144, quarter_rows, 0)

    def gat(kind, i, ref, q, to):
        zs = plane(SRC_ORDER, i)
        return pltpu.make_async_remote_copy(
            src_ref=ref.at[q, zs], dst_ref=ref.at[q, zs], send_sem=gat_s.at[kind, i], recv_sem=gat_r.at[kind, i],
            device_id=(me, to), device_id_type=MESH)

    def gat_out(kind, i):
        return (
            lambda: gat(0, i, xb, t, right), lambda: gat(1, i, xb, t, left),
            lambda: gat(2, i, db, t, right), lambda: gat(3, i, db, t, left),
            lambda: gat(4, i, xb, left, right), lambda: gat(5, i, db, right, left),
        )[kind]()

    def gat_in(kind, i):
        return (
            lambda: gat(0, i, xb, left, right), lambda: gat(1, i, xb, right, left),
            lambda: gat(2, i, db, left, right), lambda: gat(3, i, db, right, left),
            lambda: gat(4, i, xb, far, right), lambda: gat(5, i, db, far, left),
        )[kind]()

    def stage_d(i):
        zs = plane(SRC_ORDER, i)
        others(zs * PL, lambda s: a2a_in(s).wait_recv())
        got = recv[pl.ds(zs * PL, PL)].reshape(PL * SB, FP)
        xb[t, zs] = dot(cx_ref[...], got).astype(BF16)
        db[t, zs] = dot(cd_ref[...], got).astype(BF16)
        for kind in range(4):
            gat_out(kind, i).start()

    def stage_f(i):
        gat_in(0, i).wait_recv()
        gat_out(4, i).start()
        gat_in(3, i).wait_recv()
        gat_out(5, i).start()

    def rs_far(i):
        zs = plane(SRC_ORDER, i)
        return pltpu.make_async_remote_copy(
            src_ref=dxs.at[0, zs], dst_ref=far_in.at[zs], send_sem=far_s.at[i], recv_sem=far_r.at[i],
            device_id=(me, left if i % 2 == 0 else right), device_id_type=MESH)

    def rs_left(i):
        zs = plane(SRC_ORDER, i)
        return pltpu.make_async_remote_copy(
            src_ref=dxs.at[1, zs], dst_ref=right_in.at[zs], send_sem=out_s.at[0, i], recv_sem=right_r.at[i],
            device_id=(me, left), device_id_type=MESH)

    def rs_right(i):
        zs = plane(SRC_ORDER, i)
        return pltpu.make_async_remote_copy(
            src_ref=dxs.at[3, zs], dst_ref=left_in.at[zs], send_sem=out_s.at[1, i], recv_sem=left_r.at[i],
            device_id=(me, right), device_id_type=MESH)

    def stage_c(i):
        zs = plane(SRC_ORDER, i)
        for kind in (1, 2, 4, 5):
            gat_in(kind, i).wait_recv()
        acc_g[...] = jnp.zeros_like(acc_g)
        acc_u[...] = jnp.zeros_like(acc_u)
        acc_d[...] = jnp.zeros_like(acc_d)

        def forward(q, c):
            feats = pl.ds(pl.multiple_of(q * F, 16), F)
            xq = xb[q, zs, :, 0:F]
            acc_g[...] += dot(xq, wg[feats, :])
            acc_u[...] += dot(xq, wu[feats, :])
            acc_d[...] += dot_lanes(db[q, zs, :, 0:F], wdq[q, :, 0:F])
            return c

        lax.fori_loop(0, NT, forward, 0)

        def elementwise(r, c):
            rows = pl.ds(pl.multiple_of(r * 16, 16), 16)
            gate, up, back = acc_g[rows, :], acc_u[rows, :] + 1.0, acc_d[rows, :]
            p = xb[t, zs, rows, F : F + 1].astype(F32)
            sig = 1.0 / (1.0 + jnp.exp(-SLOPE * gate))
            swish = gate * sig
            active = (swish * up).astype(BF16).astype(F32)
            prob[rows, :] = jnp.broadcast_to(jnp.sum(active * back, axis=1, keepdims=True), (16, 128))
            delta = p * back
            pa[zs, rows, 0:F] = (p * active).astype(BF16)
            dg[zs, rows, 0:F] = (delta * up * (sig + SLOPE * swish * (1.0 - sig))).astype(BF16)
            du[zs, rows, 0:F] = (delta * swish).astype(BF16)
            return c

        lax.fori_loop(0, GR // 16, elementwise, 0)

        def backward(r, c):
            q = (t + 2 + r) % NT
            feats = pl.ds(pl.multiple_of(q * F, 16), F)
            part = dot_lanes(dg[zs, :, 0:F], wg[feats, :]) + dot_lanes(du[zs, :, 0:F], wu[feats, :])
            dxs[r, zs, :, 0:F] = part.astype(BF16)
            dxs[r, zs, :, F:FP] = prob[:, 0 : FP - F].astype(BF16)
            return c

        lax.fori_loop(0, NT, backward, 0)
        rs_far(i).start()
        if i % 2 == 0:
            rs_right(i).start()
        else:
            rs_left(i).start()

    def stage_s(i):
        zs = plane(SRC_ORDER, i)
        rs_far(i).wait()
        role = 1 if i % 2 == 0 else 3
        dxs[role, zs] = (dxs[role, zs].astype(F32) + far_in[zs].astype(F32)).astype(BF16)
        if i % 2 == 0:
            rs_left(i).start()
        else:
            rs_right(i).start()

    def back(s):
        return pltpu.make_async_remote_copy(
            src_ref=ret.at[s], dst_ref=ret_in.at[me], send_sem=ret_s.at[s], recv_sem=ret_r.at[me],
            device_id=(s, t), device_id_type=MESH)

    def back_in(o):
        return pltpu.make_async_remote_copy(
            src_ref=ret.at[o], dst_ref=ret_in.at[o], send_sem=ret_s.at[o], recv_sem=ret_r.at[o],
            device_id=(o, t), device_id_type=MESH)

    def stage_e(i):
        zs = plane(SRC_ORDER, i)
        rs_left(i).wait()
        rs_right(i).wait()
        total = dxs[2, zs].astype(F32) + left_in[zs].astype(F32) + right_in[zs].astype(F32)
        rows = dot(rx_ref[...], total.astype(BF16))
        for j in range(PL):
            ret[zs * PL + j] = rows[j * RB : (j + 1) * RB].astype(BF16)
        if i == 0:
            ret_in[me] = ret[me]
        others(zs * PL, lambda s: back(s).start())

    stage_d(0)
    stage_d(1)
    stage_f(0)
    stage_d(2)
    stage_f(1)
    stage_d(3)
    stage_f(2)
    stage_c(0)
    stage_f(3)
    stage_c(1)
    stage_s(0)
    stage_c(2)
    stage_s(1)
    stage_e(0)
    stage_c(3)
    outs = [
        pltpu.make_async_copy(src, dst, o_sem.at[i])
        for i, (src, dst) in enumerate(((xb, x_out), (db, d_out), (dg, dg_out), (du, du_out), (pa, pa_out)))
    ]
    for o in outs:
        o.start()
    stage_s(2)
    stage_e(1)
    stage_s(3)
    stage_e(2)
    stage_e(3)

    for i in range(G):
        for kind in range(6):
            gat_out(kind, i).wait_send()

    def finish(o, c):
        @pl.when(o != me)
        def _():
            a2a(o).wait_send()
            back(o).wait_send()
            back_in(o).wait_recv()

        return c

    lax.fori_loop(0, NDP, finish, 0)
    for o in outs:
        o.wait()
    last = pltpu.make_async_copy(ret_in, back_out, o_sem.at[5])
    last.start()
    last.wait()


def grads_kernel(
    ids_ref, pcol_ref, c24_ref, x_ref, d_ref, dg_ref, du_ref, pa_ref, back_ref,
    in_grad, gate_grad, up_grad, down_grad, prob_grad,
):
    q = pl.program_id(0)
    xq = x_ref[0, :, 0:F]
    xt = xq.T
    gate_grad[...] = dot(xt, dg_ref[:, 0:F]).astype(BF16)
    up_grad[...] = dot(xt, du_ref[:, 0:F]).astype(BF16)
    pt = pa_ref[:, 0:F].T
    piece = dot(pt, d_ref[0, :, 0:F]).astype(BF16)
    for k in range(NT):

        @pl.when(q == k)
        def _():
            down_grad[:, k * F : (k + 1) * F] = piece

    @pl.when(q == 0)
    def _():
        ids = ids_ref[...]
        table = owner_table(pcol_ref[...])
        ranks = route_ranks(ids, table)
        spread = jnp.where(iota((NDP * RB, 128), 1) == c24_ref[...], 1.0, 0.0).astype(BF16)
        slots = dot_lanes(ranks, spread)
        row = lax.broadcasted_iota(jnp.int32, (TOK, NDP * RB), 1)
        hot = jnp.where(slots == (row % RB).astype(F32), 1.0, 0.0).astype(BF16)
        sums = dot(hot, back_ref[:, 0:F])
        in_grad[...] = sums.astype(BF16)
        ones = dot(hot, jnp.where(iota((NDP * RB, 128), 1) == c24_ref[...], back_ref[:, FP - 128 :][:, 127:128].astype(F32), 0.0).astype(BF16))
        for k in range(4):
            pick = jnp.where(ids[:, k : k + 1] == iota((TOK, 128), 1), 1.0, 0.0).astype(BF16)
            mine = dot(pick, table)
            prob_grad[:, k : k + 1] = jnp.sum(mine * ones, axis=1, keepdims=True).astype(BF16)


def tables():
    r = np.arange(PL * SB)
    jj = r % SB
    jx = np.where(jj < CAP, jj, -5)
    jd = np.where((jj >= DOFF) & (jj < DOFF + CAP), jj - DOFF, -5)
    c40 = np.stack([r // SB, jx, jd], axis=1).astype(np.int32)
    cx = np.zeros((GR, PL * SB), np.float32)
    cd = np.zeros((GR, PL * SB), np.float32)
    rx = np.zeros((PL * RB, GR), np.float32)
    for j in range(PL):
        for k in range(CAP):
            cx[j * CAP + k, j * SB + k] = 1
            cd[j * CAP + k, j * SB + DOFF + k] = 1
            rx[j * RB + k, j * CAP + k] = 1
    c24 = (np.arange(NDP * RB) // RB).astype(np.int32)[:, None]
    return c40, cx, cd, rx, c24


def shards(tokens, out_grad, route_probs, expert_ids, placement_map, w_gate, w_up, w_down):
    c40, cx, cd, rx, c24 = tables()
    pcol = placement_map[:, None]
    vmem = pl.BlockSpec(memory_space=pltpu.VMEM)
    hbm = pl.BlockSpec(memory_space=pl.ANY)
    grp = jax.ShapeDtypeStruct((G, GR, FP), BF16)
    quart = jax.ShapeDtypeStruct((NT, G, GR, FP), BF16)
    dma = pltpu.SemaphoreType.DMA
    x, d, dg, du, pa, back = pl.pallas_call(
        comm_kernel,
        out_shape=(quart, quart, grp, grp, grp, jax.ShapeDtypeStruct((NDP, RB, FP), BF16)),
        in_specs=[vmem] * 9 + [hbm] * 3,
        out_specs=[hbm] * 6,
        scratch_shapes=[
            pltpu.VMEM((NDP, SB, FP), BF16), pltpu.VMEM((NDP, SB, FP), BF16),
            pltpu.VMEM((NT, G, GR, FP), BF16), pltpu.VMEM((NT, G, GR, FP), BF16),
            pltpu.VMEM((NT * F, F), BF16), pltpu.VMEM((NT * F, F), BF16), pltpu.VMEM((F, NT * F), BF16),
            pltpu.VMEM((NT, F, FP), BF16),
            pltpu.VMEM((GR, F), F32), pltpu.VMEM((GR, F), F32), pltpu.VMEM((GR, F), F32),
            pltpu.VMEM((G, GR, FP), BF16), pltpu.VMEM((G, GR, FP), BF16), pltpu.VMEM((G, GR, FP), BF16),
            pltpu.VMEM((GR, 128), F32),
            pltpu.VMEM((NT, G, GR, FP), BF16),
            pltpu.VMEM((G, GR, FP), BF16), pltpu.VMEM((G, GR, FP), BF16), pltpu.VMEM((G, GR, FP), BF16),
            pltpu.VMEM((NDP, RB, FP), BF16), pltpu.VMEM((NDP, RB, FP), BF16),
            dma((3,)), dma((NDP,)), dma((NDP,)), dma((6, G)), dma((6, G)), dma((G,)), dma((G,)),
            dma((2, G)), dma((G,)), dma((G,)), dma((NDP,)), dma((NDP,)), dma((6,)),
        ],
        compiler_params=pltpu.CompilerParams(
            collective_id=0, has_side_effects=True, vmem_limit_bytes=60 * 1024 * 1024
        ),
        name="exchange",
    )(
        expert_ids, pcol, route_probs, tokens, out_grad,
        jnp.asarray(c40), jnp.asarray(cx, BF16), jnp.asarray(cd, BF16), jnp.asarray(rx, BF16),
        w_gate[0], w_up[0], w_down[0],
    )
    rows = G * GR
    whole = lambda *s: pl.BlockSpec(s, lambda q: (0,) * len(s))
    in_grad, gate_grad, up_grad, down_grad, prob_grad = pl.pallas_call(
        grads_kernel,
        grid=(NT,),
        out_shape=(
            jax.ShapeDtypeStruct((TOK, F), BF16),
            jax.ShapeDtypeStruct((NT * F, F), BF16),
            jax.ShapeDtypeStruct((NT * F, F), BF16),
            jax.ShapeDtypeStruct((F, NT * F), BF16),
            jax.ShapeDtypeStruct((TOK, 4), BF16),
        ),
        in_specs=[
            whole(TOK, 4), whole(128, 1), whole(NDP * RB, 1),
            pl.BlockSpec((1, rows, FP), lambda q: (q, 0, 0)), pl.BlockSpec((1, rows, FP), lambda q: (q, 0, 0)),
            whole(rows, FP), whole(rows, FP), whole(rows, FP), whole(NDP * RB, FP),
        ],
        out_specs=[
            whole(TOK, F),
            pl.BlockSpec((F, F), lambda q: (q, 0)),
            pl.BlockSpec((F, F), lambda q: (q, 0)),
            whole(F, NT * F),
            whole(TOK, 4),
        ],
        compiler_params=pltpu.CompilerParams(vmem_limit_bytes=60 * 1024 * 1024),
        name="grads",
    )(
        expert_ids, pcol, jnp.asarray(c24),
        x.reshape(NT, rows, FP), d.reshape(NT, rows, FP),
        dg.reshape(rows, FP), du.reshape(rows, FP), pa.reshape(rows, FP), back.reshape(NDP * RB, FP),
    )
    return (in_grad, gate_grad[None], up_grad[None], down_grad[None], prob_grad)


def solution(mesh):
    in_specs = (
        P("dp", "tensor"), P("dp", "tensor"), P("dp", None), P("dp", None), P(),
        P("dp", None, "tensor"), P("dp", None, "tensor"), P("dp", "tensor", None),
    )
    out_specs = (
        P("dp", "tensor"), P("dp", None, "tensor"), P("dp", None, "tensor"),
        P("dp", "tensor", None), P("dp", None),
    )
    return jax.shard_map(shards, mesh=mesh, in_specs=in_specs, out_specs=out_specs, check_vma=False)
```

```python
import functools

import jax
import jax.numpy as jnp
import numpy as np
from jax import lax
from jax.experimental import pallas as pl
from jax.experimental.pallas import tpu as pltpu
from jax.sharding import PartitionSpec as P

SLOPE = 1.702
MESH = pl.DeviceIdType.MESH
NDP, NT = 32, 4
CAP = 18
TOK, F, FP = 384, 720, 768
SB, DOFF = 40, 20
RB = 24
PL = 8
G = 4
GR = PL * CAP
WR, WCH = 144, 5
NW = 640
SRC_ORDER = (0, 1, 3, 2)
DST_ORDER = (0, 3, 1, 2)
LANES = (((1,), (1,)), ((), ()))
F32, BF16 = jnp.float32, jnp.bfloat16


def dot(a, b):
    return jnp.dot(a, b, preferred_element_type=F32)


def dot_lanes(a, b):
    return lax.dot_general(a, b, LANES, preferred_element_type=F32)


def iota(shape, dim):
    return lax.broadcasted_iota(jnp.int32, shape, dim)


def owner_table(prow):
    return jnp.where(prow == 4 * iota((128, 128), 0), 1.0, 0.0).astype(BF16)


def picks(ids, k):
    return iota((128, TOK), 0) == ids[k : k + 1, :]


def route_ranks(ids, table):
    hit = jnp.zeros((128, TOK), F32)
    for k in range(4):
        hit += jnp.where(picks(ids, k), 1.0, 0.0)
    member = dot(table, hit.astype(BF16))
    earlier = jnp.where(iota((TOK, TOK), 0) < iota((TOK, TOK), 1), 1.0, 0.0).astype(BF16)
    rank = dot(member.astype(BF16), earlier)
    return jnp.where(member > 0.5, rank, -1.0).astype(BF16)


def comm_kernel(
    ids_ref, prow_ref, probs_ref, tok_ref, og_ref, c40_ref, cx_ref, cd_ref, rx_ref, wg_hbm, wu_hbm, wd_hbm,
    x_out, d_out, dgt_out, dut_out, pat_out, back_out,
    send, recv, xb, db, stage, wq, acc_g, acc_u, acc_d, dg, du, pa, prob, dxs, far_in, left_in, right_in, ret, ret_in, xf, df, dgt, dut, pat,
    w_sem, a2a_s, a2a_r, gat_s, gat_r, far_s, far_r, out_s, left_r, right_r, ret_s, ret_r, o_sem,
):
    me = lax.axis_index("dp")
    t = lax.axis_index("tensor")
    z = me // PL
    right, left, far = (t + 1) % NT, (t + 3) % NT, (t + 2) % NT

    barrier = pltpu.get_barrier_semaphore()

    def greet(d, c):
        @pl.when(d != me)
        def _():
            pl.semaphore_signal(barrier, inc=1, device_id=(d, t), device_id_type=MESH)

        return c

    lax.fori_loop(0, NDP, greet, 0)
    for nb in (left, right):
        pl.semaphore_signal(barrier, inc=1, device_id=(me, nb), device_id_type=MESH)

    weights = (wg_hbm, wu_hbm, wd_hbm)

    def load(n):
        w, r = n // WCH, n % WCH
        return pltpu.make_async_copy(
            weights[w].at[r * WR : (r + 1) * WR], stage.at[n % 3], w_sem.at[n % 3])

    for n in range(3):
        load(n).start()

    ids = ids_ref[...]
    table = owner_table(prow_ref[...])
    probs = probs_ref[...].astype(F32)
    ranks = route_ranks(ids, table)
    pw = jnp.zeros((128, TOK), F32)
    for k in range(4):
        pw += jnp.where(picks(ids, k), probs[k : k + 1, :], 0.0)
    owner_p = dot(table, pw.astype(BF16)).astype(BF16)

    def plane(order, i):
        return (z + order[i]) % G

    def build(zd):
        block, jx, jd = c40_ref[:, 0:1], c40_ref[:, 1:2], c40_ref[:, 2:3]
        mine = iota((PL * SB, 128), 1) == block + zd * PL
        slots = dot(jnp.where(mine, 1.0, 0.0).astype(BF16), ranks)
        hot_x = jnp.where(slots == jx.astype(F32), 1.0, 0.0).astype(BF16)
        hot_d = jnp.where(slots == jd.astype(F32), 1.0, 0.0).astype(BF16)
        rows = dot_lanes(hot_x, tok_ref[...]) + dot_lanes(hot_d, og_ref[...])
        p = jnp.sum(jnp.where(mine, dot_lanes(hot_x, owner_p), 0.0), axis=1, keepdims=True)
        for j in range(PL):
            part = slice(j * SB, (j + 1) * SB)
            send[zd * PL + j, :, 0:F] = rows[part].astype(BF16)
            send[zd * PL + j, :, F:FP] = jnp.broadcast_to(p[part], (SB, FP - F)).astype(BF16)

    def a2a(o):
        return pltpu.make_async_remote_copy(
            src_ref=send.at[o], dst_ref=recv.at[me], send_sem=a2a_s.at[o], recv_sem=a2a_r.at[me],
            device_id=(o, t), device_id_type=MESH)

    def a2a_in(s):
        return pltpu.make_async_remote_copy(
            src_ref=send.at[s], dst_ref=recv.at[s], send_sem=a2a_s.at[s], recv_sem=a2a_r.at[s],
            device_id=(s, t), device_id_type=MESH)

    def others(first, act):
        def body(j, c):
            o = first + j

            @pl.when(o != me)
            def _():
                act(o)

            return c

        lax.fori_loop(0, PL, body, 0)

    for i in range(G):
        zd = plane(DST_ORDER, i)
        build(zd)
        if i == 0:
            pl.semaphore_wait(barrier, NDP - 1 + 2)
            recv[me] = send[me]
        others(zd * PL, lambda o: a2a(o).start())

    def cut(w):
        for r in range(WCH):
            n = w * WCH + r
            load(n).wait()
            for q in range(NT):
                wq[w, q, r * WR : (r + 1) * WR, 0:F] = stage[n % 3, :, q * F : (q + 1) * F]
            if n + 3 < 3 * WCH:
                load(n + 3).start()

    def gat(kind, i, ref, q, to):
        zs = plane(SRC_ORDER, i)
        return pltpu.make_async_remote_copy(
            src_ref=ref.at[q, zs], dst_ref=ref.at[q, zs], send_sem=gat_s.at[kind, i], recv_sem=gat_r.at[kind, i],
            device_id=(me, to), device_id_type=MESH)

    def gat_out(kind, i):
        return (
            lambda: gat(0, i, xb, t, right), lambda: gat(1, i, xb, t, left),
            lambda: gat(2, i, db, t, right), lambda: gat(3, i, db, t, left),
            lambda: gat(4, i, xb, left, right), lambda: gat(5, i, db, right, left),
        )[kind]()

    def gat_in(kind, i):
        return (
            lambda: gat(0, i, xb, left, right), lambda: gat(1, i, xb, right, left),
            lambda: gat(2, i, db, left, right), lambda: gat(3, i, db, right, left),
            lambda: gat(4, i, xb, far, right), lambda: gat(5, i, db, far, left),
        )[kind]()

    def stage_d(i):
        zs = plane(SRC_ORDER, i)
        others(zs * PL, lambda s: a2a_in(s).wait_recv())
        got = recv[pl.ds(zs * PL, PL)].reshape(PL * SB, FP)
        xb[t, zs] = dot(cx_ref[...], got).astype(BF16)
        db[t, zs] = dot(cd_ref[...], got).astype(BF16)
        for kind in range(4):
            gat_out(kind, i).start()

    def stage_f(i):
        gat_in(0, i).wait_recv()
        gat_out(4, i).start()
        gat_in(3, i).wait_recv()
        gat_out(5, i).start()

    def rs_far(i):
        zs = plane(SRC_ORDER, i)
        return pltpu.make_async_remote_copy(
            src_ref=dxs.at[0, zs], dst_ref=far_in.at[zs], send_sem=far_s.at[i], recv_sem=far_r.at[i],
            device_id=(me, left if i % 2 == 0 else right), device_id_type=MESH)

    def rs_left(i):
        zs = plane(SRC_ORDER, i)
        return pltpu.make_async_remote_copy(
            src_ref=dxs.at[1, zs], dst_ref=right_in.at[zs], send_sem=out_s.at[0, i], recv_sem=right_r.at[i],
            device_id=(me, left), device_id_type=MESH)

    def rs_right(i):
        zs = plane(SRC_ORDER, i)
        return pltpu.make_async_remote_copy(
            src_ref=dxs.at[3, zs], dst_ref=left_in.at[zs], send_sem=out_s.at[1, i], recv_sem=left_r.at[i],
            device_id=(me, right), device_id_type=MESH)

    def stage_c(i):
        zs = plane(SRC_ORDER, i)
        for kind in (1, 2, 4, 5):
            gat_in(kind, i).wait_recv()
        acc_g[...] = jnp.zeros_like(acc_g)
        acc_u[...] = jnp.zeros_like(acc_u)
        acc_d[...] = jnp.zeros_like(acc_d)

        def forward(q, c):
            xq = xb[q, zs, :, 0:F]
            acc_g[...] += dot_lanes(xq, wq[0, q, :, 0:F])
            acc_u[...] += dot_lanes(xq, wq[1, q, :, 0:F])
            acc_d[...] += dot_lanes(db[q, zs, :, 0:F], wq[2, q, :, 0:F])
            return c

        lax.fori_loop(0, NT, forward, 0)

        def elementwise(r, c):
            rows = pl.ds(pl.multiple_of(r * 16, 16), 16)
            gate, up, back = acc_g[rows, :], acc_u[rows, :] + 1.0, acc_d[rows, :]
            p = xb[t, zs, rows, F : F + 1].astype(F32)
            sig = 1.0 / (1.0 + jnp.exp(-SLOPE * gate))
            swish = gate * sig
            active = (swish * up).astype(BF16).astype(F32)
            prob[rows, :] = jnp.broadcast_to(jnp.sum(active * back, axis=1, keepdims=True), (16, 128))
            delta = p * back
            pa[zs, rows, 0:F] = (p * active).astype(BF16)
            dg[zs, rows, 0:F] = (delta * up * (sig + SLOPE * swish * (1.0 - sig))).astype(BF16)
            du[zs, rows, 0:F] = (delta * swish).astype(BF16)
            return c

        lax.fori_loop(0, GR // 16, elementwise, 0)

        def backward(r, c):
            q = (t + 2 + r) % NT
            part = dot(dg[zs, :, 0:F], wq[0, q, :, 0:F]) + dot(du[zs, :, 0:F], wq[1, q, :, 0:F])
            dxs[r, zs, :, 0:F] = part.astype(BF16)
            dxs[r, zs, :, F:FP] = prob[:, 0 : FP - F].astype(BF16)
            return c

        lax.fori_loop(0, NT, backward, 0)
        rs_far(i).start()
        if i % 2 == 0:
            rs_right(i).start()
        else:
            rs_left(i).start()

    def stage_s(i):
        zs = plane(SRC_ORDER, i)
        rs_far(i).wait()
        role = 1 if i % 2 == 0 else 3
        dxs[role, zs] = (dxs[role, zs].astype(F32) + far_in[zs].astype(F32)).astype(BF16)
        if i % 2 == 0:
            rs_left(i).start()
        else:
            rs_right(i).start()

    def back(s):
        return pltpu.make_async_remote_copy(
            src_ref=ret.at[s], dst_ref=ret_in.at[me], send_sem=ret_s.at[s], recv_sem=ret_r.at[me],
            device_id=(s, t), device_id_type=MESH)

    def back_in(o):
        return pltpu.make_async_remote_copy(
            src_ref=ret.at[o], dst_ref=ret_in.at[o], send_sem=ret_s.at[o], recv_sem=ret_r.at[o],
            device_id=(o, t), device_id_type=MESH)

    def stage_e(i):
        zs = plane(SRC_ORDER, i)
        rs_left(i).wait()
        rs_right(i).wait()
        total = dxs[2, zs].astype(F32) + left_in[zs].astype(F32) + right_in[zs].astype(F32)
        rows = dot(rx_ref[...], total.astype(BF16))
        for j in range(PL):
            ret[zs * PL + j] = rows[j * RB : (j + 1) * RB].astype(BF16)
        if i == 0:
            ret_in[me] = ret[me]
        others(zs * PL, lambda s: back(s).start())

    def widen(i):
        zs = plane(SRC_ORDER, i)

        def body(r, c):
            rows = pl.ds(pl.multiple_of(r * 48, 16), 48)
            to = pl.ds(pl.multiple_of(zs * GR + r * 48, 16), 48)
            for q in range(NT):
                xf[to, q * F : (q + 1) * F] = xb[q, zs, rows, 0:F]
                df[to, q * F : (q + 1) * F] = db[q, zs, rows, 0:F]
            return c

        lax.fori_loop(0, GR // 48, body, 0)

    outs = [
        pltpu.make_async_copy(src, dst, o_sem.at[i])
        for i, (src, dst) in enumerate(((xf, x_out), (df, d_out), (dgt, dgt_out), (dut, dut_out), (pat, pat_out)))
    ]
    stage_d(0)
    cut(0)
    stage_d(1)
    cut(1)
    stage_f(0)
    stage_d(2)
    cut(2)
    stage_f(1)
    stage_d(3)
    stage_f(2)
    stage_c(0)
    stage_f(3)
    stage_c(1)
    stage_s(0)
    widen(0)
    stage_c(2)
    stage_s(1)
    stage_e(0)
    widen(1)
    stage_c(3)
    stage_s(2)
    stage_e(1)
    widen(2)
    stage_s(3)
    widen(3)
    outs[0].start()
    outs[1].start()
    for i, (src, dst) in enumerate(((dg, dgt), (du, dut), (pa, pat))):
        dst[...] = src[...].reshape(G * GR, FP)[:, 0:F].T
        outs[2 + i].start()
    stage_e(2)
    stage_e(3)

    for i in range(G):
        for kind in range(6):
            gat_out(kind, i).wait_send()

    def finish(o, c):
        @pl.when(o != me)
        def _():
            a2a(o).wait_send()
            back(o).wait_send()
            back_in(o).wait_recv()

        return c

    lax.fori_loop(0, NDP, finish, 0)
    for o in outs:
        o.wait()
    last = pltpu.make_async_copy(ret_in, back_out, o_sem.at[5])
    last.start()
    last.wait()


def grads_kernel(
    ids_ref, prow_ref, c24_ref, x_ref, d_ref, dgt_ref, dut_ref, pat_ref, back_ref,
    in_grad, gate_grad, up_grad, down_grad, prob_grad,
):
    x = x_ref[...]
    gate_grad[...] = dot(dgt_ref[...], x).astype(BF16)
    up_grad[...] = dot(dut_ref[...], x).astype(BF16)
    down_grad[...] = dot(pat_ref[...], d_ref[...]).astype(BF16)

    @pl.when(pl.program_id(0) == 0)
    def _():
        ids = ids_ref[...]
        table = owner_table(prow_ref[...])
        ranks = route_ranks(ids, table)
        mine = iota((NDP * RB, 128), 1) == c24_ref[:, 0:1]
        slots = dot(jnp.where(mine, 1.0, 0.0).astype(BF16), ranks)
        hot = jnp.where(slots == c24_ref[:, 1:2].astype(F32), 1.0, 0.0).astype(BF16)
        in_grad[...] = dot(back_ref[:, 0:F].T, hot).astype(BF16)
        prob = jnp.where(mine, back_ref[:, FP - 128 :][:, 127:128].astype(F32), 0.0).astype(BF16)
        by_owner = dot(prob.T, hot)
        for k in range(4):
            owner = dot(table, jnp.where(picks(ids, k), 1.0, 0.0).astype(BF16))
            prob_grad[k : k + 1, :] = jnp.sum(owner * by_owner, axis=0, keepdims=True).astype(BF16)


def tables():
    r = np.arange(PL * SB)
    jj = r % SB
    jx = np.where(jj < CAP, jj, -5)
    jd = np.where((jj >= DOFF) & (jj < DOFF + CAP), jj - DOFF, -5)
    c40 = np.stack([r // SB, jx, jd], axis=1).astype(np.int32)
    cx = np.zeros((GR, PL * SB), np.float32)
    cd = np.zeros((GR, PL * SB), np.float32)
    rx = np.zeros((PL * RB, GR), np.float32)
    for j in range(PL):
        for k in range(CAP):
            cx[j * CAP + k, j * SB + k] = 1
            cd[j * CAP + k, j * SB + DOFF + k] = 1
            rx[j * RB + k, j * CAP + k] = 1
    r = np.arange(NDP * RB)
    c24 = np.stack([r // RB, r % RB], axis=1).astype(np.int32)
    return c40, cx, cd, rx, c24


def shards(tokens, out_grad, route_probs, expert_ids, placement_map, w_gate, w_up, w_down):
    c40, cx, cd, rx, c24 = tables()
    ids, prow = expert_ids.T, placement_map[None, :]
    vmem = pl.BlockSpec(memory_space=pltpu.VMEM)
    hbm = pl.BlockSpec(memory_space=pl.ANY)
    turned = jax.ShapeDtypeStruct((F, G * GR), BF16)
    wide = jax.ShapeDtypeStruct((G * GR, NT * F), BF16)
    dma = pltpu.SemaphoreType.DMA
    x, d, dgt, dut, pat, back = pl.pallas_call(
        comm_kernel,
        out_shape=(wide, wide, turned, turned, turned, jax.ShapeDtypeStruct((NDP, RB, FP), BF16)),
        in_specs=[vmem] * 9 + [hbm] * 3,
        out_specs=[hbm] * 6,
        scratch_shapes=[
            pltpu.VMEM((NDP, SB, FP), BF16), pltpu.VMEM((NDP, SB, FP), BF16),
            pltpu.VMEM((NT, G, GR, FP), BF16), pltpu.VMEM((NT, G, GR, FP), BF16),
            pltpu.VMEM((3, WR, NT * F), BF16), pltpu.VMEM((3, NT, F, FP), BF16),
            pltpu.VMEM((GR, F), F32), pltpu.VMEM((GR, F), F32), pltpu.VMEM((GR, F), F32),
            pltpu.VMEM((G, GR, FP), BF16), pltpu.VMEM((G, GR, FP), BF16), pltpu.VMEM((G, GR, FP), BF16),
            pltpu.VMEM((GR, 128), F32),
            pltpu.VMEM((NT, G, GR, FP), BF16),
            pltpu.VMEM((G, GR, FP), BF16), pltpu.VMEM((G, GR, FP), BF16), pltpu.VMEM((G, GR, FP), BF16),
            pltpu.VMEM((NDP, RB, FP), BF16), pltpu.VMEM((NDP, RB, FP), BF16),
            pltpu.VMEM((G * GR, NT * F), BF16), pltpu.VMEM((G * GR, NT * F), BF16),
            pltpu.VMEM((F, G * GR), BF16), pltpu.VMEM((F, G * GR), BF16), pltpu.VMEM((F, G * GR), BF16),
            dma((3,)), dma((NDP,)), dma((NDP,)), dma((6, G)), dma((6, G)), dma((G,)), dma((G,)),
            dma((2, G)), dma((G,)), dma((G,)), dma((NDP,)), dma((NDP,)), dma((6,)),
        ],
        compiler_params=pltpu.CompilerParams(
            collective_id=0, has_side_effects=True, vmem_limit_bytes=60 * 1024 * 1024
        ),
        name="exchange",
    )(
        ids, prow, route_probs.T, tokens.T, out_grad.T,
        jnp.asarray(c40), jnp.asarray(cx, BF16), jnp.asarray(cd, BF16), jnp.asarray(rx, BF16),
        w_gate[0].T, w_up[0].T, w_down[0],
    )
    rows = G * GR
    whole = lambda *s: pl.BlockSpec(s, lambda n: (0,) * len(s))
    strip = lambda r: pl.BlockSpec((r, NW), lambda n: (0, n))
    grad = jax.ShapeDtypeStruct((F, NT * F), BF16)
    in_grad, gate_grad, up_grad, down_grad, prob_grad = pl.pallas_call(
        grads_kernel,
        grid=(-(-NT * F // NW),),
        out_shape=(
            jax.ShapeDtypeStruct((F, TOK), BF16), grad, grad, grad, jax.ShapeDtypeStruct((4, TOK), BF16),
        ),
        in_specs=[
            whole(4, TOK), whole(1, 128), whole(NDP * RB, 2), strip(rows), strip(rows),
            whole(F, rows), whole(F, rows), whole(F, rows), whole(NDP * RB, FP),
        ],
        out_specs=[whole(F, TOK), strip(F), strip(F), strip(F), whole(4, TOK)],
        compiler_params=pltpu.CompilerParams(vmem_limit_bytes=60 * 1024 * 1024),
        name="grads",
    )(ids, prow, jnp.asarray(c24), x, d, dgt, dut, pat, back.reshape(NDP * RB, FP))
    return (in_grad.T, gate_grad.T[None], up_grad.T[None], down_grad[None], prob_grad.T)


def solution(mesh):
    in_specs = (
        P("dp", "tensor"), P("dp", "tensor"), P("dp", None), P("dp", None), P(),
        P("dp", None, "tensor"), P("dp", None, "tensor"), P("dp", "tensor", None),
    )
    out_specs = (
        P("dp", "tensor"), P("dp", None, "tensor"), P("dp", None, "tensor"),
        P("dp", "tensor", None), P("dp", None),
    )
    return jax.shard_map(shards, mesh=mesh, in_specs=in_specs, out_specs=out_specs, check_vma=False)
```

```python
import functools

import jax
import jax.numpy as jnp
import numpy as np
from jax import lax
from jax.experimental import pallas as pl
from jax.experimental.pallas import tpu as pltpu
from jax.sharding import PartitionSpec as P

SLOPE = 1.702
MESH = pl.DeviceIdType.MESH
NDP, NT = 32, 4
CAP = 18
TOK, F, FP = 384, 720, 768
SB, DOFF = 40, 20
RB = 24
PL = 8
G = 4
GR = PL * CAP
WR, WCH = 144, 5
EXCHANGE_VMEM, COMBINE_VMEM = 48 * 2**20, 16 * 2**20
SRC_ORDER = (0, 1, 3, 2)
DST_ORDER = (0, 3, 1, 2)
LANES = (((1,), (1,)), ((), ()))
F32, BF16 = jnp.float32, jnp.bfloat16


def dot(a, b):
    return jnp.dot(a, b, preferred_element_type=F32)


def dot_lanes(a, b):
    return lax.dot_general(a, b, LANES, preferred_element_type=F32)


def iota(shape, dim):
    return lax.broadcasted_iota(jnp.int32, shape, dim)


def owner_table(prow):
    return jnp.where(prow == 4 * iota((128, 128), 0), 1.0, 0.0).astype(BF16)


def picks(ids, k):
    return iota((128, TOK), 0) == ids[k : k + 1, :]


def route_ranks(ids, table):
    hit = jnp.zeros((128, TOK), F32)
    for k in range(4):
        hit += jnp.where(picks(ids, k), 1.0, 0.0)
    member = dot(table, hit.astype(BF16))
    earlier = jnp.where(iota((TOK, TOK), 0) < iota((TOK, TOK), 1), 1.0, 0.0).astype(BF16)
    rank = dot(member.astype(BF16), earlier)
    return jnp.where(member > 0.5, rank, -1.0).astype(BF16)


def comm_kernel(
    ids_ref, prow_ref, probs_ref, tok_ref, og_ref, c40_ref, cx_ref, cd_ref, rx_ref, wg_hbm, wu_hbm, wd_hbm,
    grads, back_out,
    send, recv, xd, stage, wq, acc_g, acc_u, acc_d, fac, prob, dxs, far_in, left_in, right_in, ret, ret_in, turned,
    w_sem, a2a_s, a2a_r, gat_s, gat_r, far_s, far_r, out_s, left_r, right_r, ret_s, ret_r,
):
    me = lax.axis_index("dp")
    t = lax.axis_index("tensor")
    z = me // PL
    right, left, far = (t + 1) % NT, (t + 3) % NT, (t + 2) % NT

    xb, db = xd.at[0], xd.at[1]
    dg, du, pa = fac.at[0], fac.at[1], fac.at[2]

    barrier = pltpu.get_barrier_semaphore()

    def greet(d, c):
        @pl.when(d != me)
        def _():
            pl.semaphore_signal(barrier, inc=1, device_id=(d, t), device_id_type=MESH)

        return c

    lax.fori_loop(0, NDP, greet, 0)
    for nb in (left, right):
        pl.semaphore_signal(barrier, inc=1, device_id=(me, nb), device_id_type=MESH)

    weights = (wg_hbm, wu_hbm, wd_hbm)

    def load(n):
        w, r = n // WCH, n % WCH
        return pltpu.make_async_copy(
            weights[w].at[r * WR : (r + 1) * WR], stage.at[n % 3], w_sem.at[n % 3])

    for n in range(3):
        load(n).start()

    ids = ids_ref[...]
    table = owner_table(prow_ref[...])
    probs = probs_ref[...].astype(F32)
    ranks = route_ranks(ids, table)
    pw = jnp.zeros((128, TOK), F32)
    for k in range(4):
        pw += jnp.where(picks(ids, k), probs[k : k + 1, :], 0.0)
    owner_p = dot(table, pw.astype(BF16)).astype(BF16)

    def plane(order, i):
        return (z + order[i]) % G

    def build(zd):
        block, jx, jd = c40_ref[:, 0:1], c40_ref[:, 1:2], c40_ref[:, 2:3]
        mine = iota((PL * SB, 128), 1) == block + zd * PL
        slots = dot(jnp.where(mine, 1.0, 0.0).astype(BF16), ranks)
        hot_x = jnp.where(slots == jx.astype(F32), 1.0, 0.0).astype(BF16)
        hot_d = jnp.where(slots == jd.astype(F32), 1.0, 0.0).astype(BF16)
        rows = dot_lanes(hot_x, tok_ref[...]) + dot_lanes(hot_d, og_ref[...])
        p = jnp.sum(jnp.where(mine, dot_lanes(hot_x, owner_p), 0.0), axis=1, keepdims=True)
        for j in range(PL):
            part = slice(j * SB, (j + 1) * SB)
            send[zd * PL + j, :, 0:F] = rows[part].astype(BF16)
            send[zd * PL + j, :, F:FP] = jnp.broadcast_to(p[part], (SB, FP - F)).astype(BF16)

    def a2a(o):
        return pltpu.make_async_remote_copy(
            src_ref=send.at[o], dst_ref=recv.at[me], send_sem=a2a_s.at[o], recv_sem=a2a_r.at[me],
            device_id=(o, t), device_id_type=MESH)

    def a2a_in(s):
        return pltpu.make_async_remote_copy(
            src_ref=send.at[s], dst_ref=recv.at[s], send_sem=a2a_s.at[s], recv_sem=a2a_r.at[s],
            device_id=(s, t), device_id_type=MESH)

    def others(first, act):
        def body(j, c):
            o = first + j

            @pl.when(o != me)
            def _():
                act(o)

            return c

        lax.fori_loop(0, PL, body, 0)

    for i in range(G):
        zd = plane(DST_ORDER, i)
        build(zd)
        if i == 0:
            pl.semaphore_wait(barrier, NDP - 1 + 2)
            recv[me] = send[me]
        others(zd * PL, lambda o: a2a(o).start())

    def cut(w):
        for r in range(WCH):
            n = w * WCH + r
            load(n).wait()
            for q in range(NT):
                wq[w, q, r * WR : (r + 1) * WR, 0:F] = stage[n % 3, :, q * F : (q + 1) * F]
            if n + 3 < 3 * WCH:
                load(n + 3).start()

    def gat(kind, i, ref, q, to):
        zs = plane(SRC_ORDER, i)
        return pltpu.make_async_remote_copy(
            src_ref=ref.at[q, zs], dst_ref=ref.at[q, zs], send_sem=gat_s.at[kind, i], recv_sem=gat_r.at[kind, i],
            device_id=(me, to), device_id_type=MESH)

    def gat_out(kind, i):
        return (
            lambda: gat(0, i, xb, t, right), lambda: gat(1, i, xb, t, left),
            lambda: gat(2, i, db, t, right), lambda: gat(3, i, db, t, left),
            lambda: gat(4, i, xb, left, right), lambda: gat(5, i, db, right, left),
        )[kind]()

    def gat_in(kind, i):
        return (
            lambda: gat(0, i, xb, left, right), lambda: gat(1, i, xb, right, left),
            lambda: gat(2, i, db, left, right), lambda: gat(3, i, db, right, left),
            lambda: gat(4, i, xb, far, right), lambda: gat(5, i, db, far, left),
        )[kind]()

    def stage_d(i):
        zs = plane(SRC_ORDER, i)
        others(zs * PL, lambda s: a2a_in(s).wait_recv())
        got = recv[pl.ds(zs * PL, PL)].reshape(PL * SB, FP)
        xb[t, zs] = dot(cx_ref[...], got).astype(BF16)
        db[t, zs] = dot(cd_ref[...], got).astype(BF16)
        for kind in range(4):
            gat_out(kind, i).start()

    def stage_f(i):
        gat_in(0, i).wait_recv()
        gat_out(4, i).start()
        gat_in(3, i).wait_recv()
        gat_out(5, i).start()

    def rs_far(i):
        zs = plane(SRC_ORDER, i)
        return pltpu.make_async_remote_copy(
            src_ref=dxs.at[0, zs], dst_ref=far_in.at[zs], send_sem=far_s.at[i], recv_sem=far_r.at[i],
            device_id=(me, left if i % 2 == 0 else right), device_id_type=MESH)

    def rs_left(i):
        zs = plane(SRC_ORDER, i)
        return pltpu.make_async_remote_copy(
            src_ref=dxs.at[1, zs], dst_ref=right_in.at[zs], send_sem=out_s.at[0, i], recv_sem=right_r.at[i],
            device_id=(me, left), device_id_type=MESH)

    def rs_right(i):
        zs = plane(SRC_ORDER, i)
        return pltpu.make_async_remote_copy(
            src_ref=dxs.at[3, zs], dst_ref=left_in.at[zs], send_sem=out_s.at[1, i], recv_sem=left_r.at[i],
            device_id=(me, right), device_id_type=MESH)

    def stage_c(i):
        zs = plane(SRC_ORDER, i)
        for kind in (1, 2, 4, 5):
            gat_in(kind, i).wait_recv()
        acc_g[...] = jnp.zeros_like(acc_g)
        acc_u[...] = jnp.zeros_like(acc_u)
        acc_d[...] = jnp.zeros_like(acc_d)

        def forward(q, c):
            xq = xb[q, zs, :, 0:F]
            acc_g[...] += dot_lanes(xq, wq[0, q, :, 0:F])
            acc_u[...] += dot_lanes(xq, wq[1, q, :, 0:F])
            acc_d[...] += dot_lanes(db[q, zs, :, 0:F], wq[2, q, :, 0:F])
            return c

        lax.fori_loop(0, NT, forward, 0)

        def elementwise(r, c):
            rows = pl.ds(pl.multiple_of(r * 16, 16), 16)
            gate, up, back = acc_g[rows, :], acc_u[rows, :] + 1.0, acc_d[rows, :]
            p = xb[t, zs, rows, F : F + 1].astype(F32)
            sig = 1.0 / (1.0 + jnp.exp(-SLOPE * gate))
            swish = gate * sig
            active = (swish * up).astype(BF16).astype(F32)
            prob[rows, :] = jnp.broadcast_to(jnp.sum(active * back, axis=1, keepdims=True), (16, 128))
            delta = p * back
            pa[zs, rows, 0:F] = (p * active).astype(BF16)
            dg[zs, rows, 0:F] = (delta * up * (sig + SLOPE * swish * (1.0 - sig))).astype(BF16)
            du[zs, rows, 0:F] = (delta * swish).astype(BF16)
            return c

        lax.fori_loop(0, GR // 16, elementwise, 0)

        def backward(r, c):
            q = (t + 2 + r) % NT
            part = dot(dg[zs, :, 0:F], wq[0, q, :, 0:F]) + dot(du[zs, :, 0:F], wq[1, q, :, 0:F])
            dxs[r, zs, :, 0:F] = part.astype(BF16)
            dxs[r, zs, :, F:FP] = prob[:, 0 : FP - F].astype(BF16)
            return c

        lax.fori_loop(0, NT, backward, 0)
        rs_far(i).start()
        if i % 2 == 0:
            rs_right(i).start()
        else:
            rs_left(i).start()

    def stage_s(i):
        zs = plane(SRC_ORDER, i)
        rs_far(i).wait()
        role = 1 if i % 2 == 0 else 3
        dxs[role, zs] = (dxs[role, zs].astype(F32) + far_in[zs].astype(F32)).astype(BF16)
        if i % 2 == 0:
            rs_left(i).start()
        else:
            rs_right(i).start()

    def back(s):
        return pltpu.make_async_remote_copy(
            src_ref=ret.at[s], dst_ref=ret_in.at[me], send_sem=ret_s.at[s], recv_sem=ret_r.at[me],
            device_id=(s, t), device_id_type=MESH)

    def back_in(o):
        return pltpu.make_async_remote_copy(
            src_ref=ret.at[o], dst_ref=ret_in.at[o], send_sem=ret_s.at[o], recv_sem=ret_r.at[o],
            device_id=(o, t), device_id_type=MESH)

    def stage_e(i):
        zs = plane(SRC_ORDER, i)
        rs_left(i).wait()
        rs_right(i).wait()
        total = dxs[2, zs].astype(F32) + left_in[zs].astype(F32) + right_in[zs].astype(F32)
        rows = dot(rx_ref[...], total.astype(BF16))
        for j in range(PL):
            ret[zs * PL + j] = rows[j * RB : (j + 1) * RB].astype(BF16)
        if i == 0:
            ret_in[me] = ret[me]
        others(zs * PL, lambda s: back(s).start())

    def turn(w):
        turned[w] = fac[w].reshape(G * GR, FP)[:, 0:F].T

    def grad(w, quarters):
        for q in quarters:
            rows = xd[w // 2, q].reshape(G * GR, FP)[:, 0:F]
            grads[w, :, q * F : (q + 1) * F] = dot(turned[w], rows).astype(BF16)

    stage_d(0)
    stage_d(1)
    cut(0)
    stage_f(0)
    stage_d(2)
    stage_f(1)
    cut(1)
    stage_d(3)
    cut(2)
    stage_c(0)
    stage_f(2)
    stage_c(1)
    stage_f(3)
    stage_s(0)
    stage_c(2)
    stage_s(1)
    stage_c(3)
    stage_e(0)
    stage_s(2)
    stage_e(1)
    turn(0)
    grad(0, (0,))
    grad(0, (1,))
    turn(1)
    stage_s(3)
    grad(0, (2,))
    grad(0, (3,))
    grad(1, (0,))
    stage_e(2)
    turn(2)
    grad(1, (1,))
    stage_e(3)
    grad(1, (2,))
    grad(1, (3,))
    grad(2, (0,))
    grad(2, (1,))
    grad(2, (2,))
    grad(2, (3,))

    for i in range(G):
        for kind in range(6):
            gat_out(kind, i).wait_send()

    def finish(o, c):
        @pl.when(o != me)
        def _():
            a2a(o).wait_send()
            back(o).wait_send()
            back_in(o).wait_recv()

        return c

    lax.fori_loop(0, NDP, finish, 0)

    def hand_on(o, c):
        back_out[o] = ret_in[o]
        return c

    lax.fori_loop(0, NDP, hand_on, 0)


def combine_kernel(
    ids_ref, prow_ref, c24_ref, back_ref, grads, in_grad, gate_grad, up_grad, down_grad, prob_grad, sem
):
    writes = [
        pltpu.make_async_copy(grads.at[w], dst, sem.at[w]) for w, dst in enumerate((gate_grad, up_grad, down_grad))
    ]
    for w in writes:
        w.start()
    ids = ids_ref[...]
    table = owner_table(prow_ref[...])
    ranks = route_ranks(ids, table)
    mine = iota((NDP * RB, 128), 1) == c24_ref[:, 0:1]
    slots = dot(jnp.where(mine, 1.0, 0.0).astype(BF16), ranks)
    hot = jnp.where(slots == c24_ref[:, 1:2].astype(F32), 1.0, 0.0).astype(BF16)
    in_grad[...] = dot(back_ref[:, 0:F].T, hot).astype(BF16)
    prob = jnp.where(mine, back_ref[:, FP - 128 :][:, 127:128].astype(F32), 0.0).astype(BF16)
    by_owner = dot(prob.T, hot)
    for k in range(4):
        owner = dot(table, jnp.where(picks(ids, k), 1.0, 0.0).astype(BF16))
        prob_grad[k : k + 1, :] = jnp.sum(owner * by_owner, axis=0, keepdims=True).astype(BF16)
    for w in writes:
        w.wait()


def tables():
    r = np.arange(PL * SB)
    jj = r % SB
    jx = np.where(jj < CAP, jj, -5)
    jd = np.where((jj >= DOFF) & (jj < DOFF + CAP), jj - DOFF, -5)
    c40 = np.stack([r // SB, jx, jd], axis=1).astype(np.int32)
    cx = np.zeros((GR, PL * SB), np.float32)
    cd = np.zeros((GR, PL * SB), np.float32)
    rx = np.zeros((PL * RB, GR), np.float32)
    for j in range(PL):
        for k in range(CAP):
            cx[j * CAP + k, j * SB + k] = 1
            cd[j * CAP + k, j * SB + DOFF + k] = 1
            rx[j * RB + k, j * CAP + k] = 1
    r = np.arange(NDP * RB)
    c24 = np.stack([r // RB, r % RB], axis=1).astype(np.int32)
    return c40, cx, cd, rx, c24


def shards(tokens, out_grad, route_probs, expert_ids, placement_map, w_gate, w_up, w_down):
    c40, cx, cd, rx, c24 = tables()
    ids, prow = expert_ids.T, placement_map[None, :]
    vmem = pl.BlockSpec(memory_space=pltpu.VMEM)
    hbm = pl.BlockSpec(memory_space=pl.ANY)
    turned = jax.ShapeDtypeStruct((F, G * GR), BF16)
    dma = pltpu.SemaphoreType.DMA
    grads, back = pl.pallas_call(
        comm_kernel,
        out_shape=(pltpu.VMEM((3, F, NT * F), BF16), pltpu.VMEM((NDP, RB, FP), BF16)),
        in_specs=[vmem] * 9 + [hbm] * 3,
        out_specs=[vmem, vmem],
        scratch_shapes=[
            pltpu.VMEM((NDP, SB, FP), BF16), pltpu.VMEM((NDP, SB, FP), BF16),
            pltpu.VMEM((2, NT, G, GR, FP), BF16),
            pltpu.VMEM((3, WR, NT * F), BF16), pltpu.VMEM((3, NT, F, FP), BF16),
            pltpu.VMEM((GR, F), F32), pltpu.VMEM((GR, F), F32), pltpu.VMEM((GR, F), F32),
            pltpu.VMEM((3, G, GR, FP), BF16),
            pltpu.VMEM((GR, 128), F32),
            pltpu.VMEM((NT, G, GR, FP), BF16),
            pltpu.VMEM((G, GR, FP), BF16), pltpu.VMEM((G, GR, FP), BF16), pltpu.VMEM((G, GR, FP), BF16),
            pltpu.VMEM((NDP, RB, FP), BF16), pltpu.VMEM((NDP, RB, FP), BF16),
            pltpu.VMEM((3, F, G * GR), BF16),
            dma((3,)), dma((NDP,)), dma((NDP,)), dma((6, G)), dma((6, G)), dma((G,)), dma((G,)),
            dma((2, G)), dma((G,)), dma((G,)), dma((NDP,)), dma((NDP,)),
        ],
        compiler_params=pltpu.CompilerParams(
            collective_id=0, has_side_effects=True, vmem_limit_bytes=EXCHANGE_VMEM
        ),
        name="exchange",
    )(
        ids, prow, route_probs.T, tokens.T, out_grad.T,
        jnp.asarray(c40), jnp.asarray(cx, BF16), jnp.asarray(cd, BF16), jnp.asarray(rx, BF16),
        w_gate[0].T, w_up[0].T, w_down[0],
    )
    grad = jax.ShapeDtypeStruct((F, NT * F), BF16)
    in_grad, gate_grad, up_grad, down_grad, prob_grad = pl.pallas_call(
        combine_kernel,
        out_shape=(
            jax.ShapeDtypeStruct((F, TOK), BF16), grad, grad, grad, jax.ShapeDtypeStruct((4, TOK), BF16),
        ),
        in_specs=[vmem] * 5,
        out_specs=[vmem, hbm, hbm, hbm, vmem],
        scratch_shapes=[dma((3,))],
        compiler_params=pltpu.CompilerParams(vmem_limit_bytes=COMBINE_VMEM),
        name="combine",
    )(ids, prow, jnp.asarray(c24), back.reshape(NDP * RB, FP), grads)
    return (in_grad.T, gate_grad.T[None], up_grad.T[None], down_grad[None], prob_grad.T)


def solution(mesh):
    in_specs = (
        P("dp", "tensor"), P("dp", "tensor"), P("dp", None), P("dp", None), P(),
        P("dp", None, "tensor"), P("dp", None, "tensor"), P("dp", "tensor", None),
    )
    out_specs = (
        P("dp", "tensor"), P("dp", None, "tensor"), P("dp", None, "tensor"),
        P("dp", "tensor", None), P("dp", None),
    )
    return jax.shard_map(shards, mesh=mesh, in_specs=in_specs, out_specs=out_specs, check_vma=False)
```

```python
import functools

import jax
import jax.numpy as jnp
import numpy as np
from jax import lax
from jax.experimental import pallas as pl
from jax.experimental.pallas import tpu as pltpu
from jax.sharding import PartitionSpec as P

SLOPE = 1.702
MESH = pl.DeviceIdType.MESH
NDP, NT = 32, 4
CAP = 18
TOK, F, FP = 384, 720, 768
SB, DOFF = 40, 20
RB = 24
PL = 8
G = 4
GR = PL * CAP
WR, WCH = 144, 5
EXCHANGE_VMEM, COMBINE_VMEM = 48 * 2**20, 16 * 2**20
NEAR = (
    ((0, 0), (0, 1), (0, 3), (1, 0)),
    ((1, 1), (1, 3), (3, 1), (3, 3)),
    ((2, 1), (2, 3), (1, 2), (3, 2)),
    ((2, 2), (0, 2), (2, 0), (3, 0)),
)
LANES = (((1,), (1,)), ((), ()))
F32, BF16 = jnp.float32, jnp.bfloat16


def dot(a, b):
    return jnp.dot(a, b, preferred_element_type=F32)


def dot_lanes(a, b):
    return lax.dot_general(a, b, LANES, preferred_element_type=F32)


def iota(shape, dim):
    return lax.broadcasted_iota(jnp.int32, shape, dim)


def owner_table(prow):
    return jnp.where(prow == 4 * iota((128, 128), 0), 1.0, 0.0).astype(BF16)


def picks(ids, k):
    return iota((128, TOK), 0) == ids[k : k + 1, :]


def route_ranks(ids, table):
    hit = jnp.zeros((128, TOK), F32)
    for k in range(4):
        hit += jnp.where(picks(ids, k), 1.0, 0.0)
    member = dot(table, hit.astype(BF16))
    earlier = jnp.where(iota((TOK, TOK), 0) < iota((TOK, TOK), 1), 1.0, 0.0).astype(BF16)
    rank = dot(member.astype(BF16), earlier)
    return jnp.where(member > 0.5, rank, -1.0).astype(BF16)


def comm_kernel(
    ids_ref, prow_ref, probs_ref, tok_ref, og_ref, c40_ref, cx_ref, cd_ref, rx_ref, wg_hbm, wu_hbm, wd_hbm,
    grads, back_out,
    send, recv, xd, stage, wq, acc_g, acc_u, acc_d, fac, prob, dxs, far_in, left_in, right_in, ret, ret_in, turned,
    w_sem, a2a_s, a2a_r, gat_s, gat_r, far_s, far_r, out_s, left_r, right_r, ret_s, ret_r,
):
    me = lax.axis_index("dp")
    t = lax.axis_index("tensor")
    z, y, core = me // 8, me // 2 % 4, me % 2
    right, left, far = (t + 1) % NT, (t + 3) % NT, (t + 2) % NT

    xb, db = xd.at[0], xd.at[1]
    dg, du, pa = fac.at[0], fac.at[1], fac.at[2]

    barrier = pltpu.get_barrier_semaphore()

    def greet(d, c):
        @pl.when(d != me)
        def _():
            pl.semaphore_signal(barrier, inc=1, device_id=(d, t), device_id_type=MESH)

        return c

    lax.fori_loop(0, NDP, greet, 0)
    for nb in (left, right):
        pl.semaphore_signal(barrier, inc=1, device_id=(me, nb), device_id_type=MESH)

    weights = (wg_hbm, wu_hbm, wd_hbm)

    def load(n):
        w, r = n // WCH, n % WCH
        return pltpu.make_async_copy(
            weights[w].at[r * WR : (r + 1) * WR], stage.at[n % 3], w_sem.at[n % 3])

    for n in range(3):
        load(n).start()

    ids = ids_ref[...]
    table = owner_table(prow_ref[...])
    probs = probs_ref[...].astype(F32)
    ranks = route_ranks(ids, table)
    pw = jnp.zeros((128, TOK), F32)
    for k in range(4):
        pw += jnp.where(picks(ids, k), probs[k : k + 1, :], 0.0)
    owner_p = dot(table, pw.astype(BF16)).astype(BF16)

    def source(i, j):
        dz, dy = NEAR[i][j // 2]
        return (z + dz) % 4 * 8 + (y + dy) % 4 * 2 + j % 2

    def dest(i, j):
        dz, dy = NEAR[i][j // 2]
        return (z + 4 - dz) % 4 * 8 + (y + 4 - dy) % 4 * 2 + j % 2

    def others(i, act):
        for j in range(PL):
            if i == 0 and j < 2:
                pl.when(core != j)(functools.partial(act, j))
            else:
                act(j)

    def own(at):
        for j in range(2):
            pl.when(core == j)(functools.partial(at, j))

    def build(i):
        jx, jd = c40_ref[:, 0:1], c40_ref[:, 1:2]
        dz, dy, cores = (c40_ref[:, 2 + 3 * i + k : 3 + 3 * i + k] for k in range(3))
        block = ((z - dz) & 3) * 8 + ((y - dy) & 3) * 2 + cores
        mine = iota((PL * SB, 128), 1) == block
        slots = dot(jnp.where(mine, 1.0, 0.0).astype(BF16), ranks)
        hot_x = jnp.where(slots == jx.astype(F32), 1.0, 0.0).astype(BF16)
        hot_d = jnp.where(slots == jd.astype(F32), 1.0, 0.0).astype(BF16)
        rows = dot_lanes(hot_x, tok_ref[...]) + dot_lanes(hot_d, og_ref[...])
        p = jnp.sum(jnp.where(mine, dot_lanes(hot_x, owner_p), 0.0), axis=1, keepdims=True)
        for j in range(PL):
            part = slice(j * SB, (j + 1) * SB)
            send[i * PL + j, :, 0:F] = rows[part].astype(BF16)
            send[i * PL + j, :, F:FP] = jnp.broadcast_to(p[part], (SB, FP - F)).astype(BF16)

    def a2a(i, j):
        return pltpu.make_async_remote_copy(
            src_ref=send.at[i * PL + j], dst_ref=recv.at[i * PL + j // 2 * 2 + core],
            send_sem=a2a_s.at[i * PL + j], recv_sem=a2a_r.at[i * PL + j // 2 * 2 + core],
            device_id=(dest(i, j), t), device_id_type=MESH)

    def a2a_in(i, j):
        return pltpu.make_async_remote_copy(
            src_ref=send.at[i * PL + j], dst_ref=recv.at[i * PL + j],
            send_sem=a2a_s.at[i * PL + j], recv_sem=a2a_r.at[i * PL + j],
            device_id=(source(i, j), t), device_id_type=MESH)

    def stage_b(i):
        build(i)
        if i == 0:
            pl.semaphore_wait(barrier, NDP - 1 + 2)

            def keep(j):
                recv[j] = send[j]

            own(keep)
        others(i, lambda j: a2a(i, j).start())

    def cut(w):
        for r in range(WCH):
            n = w * WCH + r
            load(n).wait()
            for q in range(NT):
                wq[w, q, r * WR : (r + 1) * WR, 0:F] = stage[n % 3, :, q * F : (q + 1) * F]
            if n + 3 < 3 * WCH:
                load(n + 3).start()

    def gat(kind, i, ref, q, to):
        zs = i
        return pltpu.make_async_remote_copy(
            src_ref=ref.at[q, zs], dst_ref=ref.at[q, zs], send_sem=gat_s.at[kind, i], recv_sem=gat_r.at[kind, i],
            device_id=(me, to), device_id_type=MESH)

    def gat_out(kind, i):
        return (
            lambda: gat(0, i, xb, t, right), lambda: gat(1, i, xb, t, left),
            lambda: gat(2, i, db, t, right), lambda: gat(3, i, db, t, left),
            lambda: gat(4, i, xb, left, right), lambda: gat(5, i, db, right, left),
        )[kind]()

    def gat_in(kind, i):
        return (
            lambda: gat(0, i, xb, left, right), lambda: gat(1, i, xb, right, left),
            lambda: gat(2, i, db, left, right), lambda: gat(3, i, db, right, left),
            lambda: gat(4, i, xb, far, right), lambda: gat(5, i, db, far, left),
        )[kind]()

    def stage_d(i):
        zs = i
        others(i, lambda j: a2a_in(i, j).wait_recv())
        got = recv[i * PL : (i + 1) * PL].reshape(PL * SB, FP)
        xb[t, zs] = dot(cx_ref[...], got).astype(BF16)
        db[t, zs] = dot(cd_ref[...], got).astype(BF16)
        for kind in range(4):
            gat_out(kind, i).start()

    def stage_f(i):
        gat_in(0, i).wait_recv()
        gat_out(4, i).start()
        gat_in(3, i).wait_recv()
        gat_out(5, i).start()

    def rs_far(i):
        zs = i
        return pltpu.make_async_remote_copy(
            src_ref=dxs.at[0, zs], dst_ref=far_in.at[zs], send_sem=far_s.at[i], recv_sem=far_r.at[i],
            device_id=(me, left if i % 2 == 0 else right), device_id_type=MESH)

    def rs_left(i):
        zs = i
        return pltpu.make_async_remote_copy(
            src_ref=dxs.at[1, zs], dst_ref=right_in.at[zs], send_sem=out_s.at[0, i], recv_sem=right_r.at[i],
            device_id=(me, left), device_id_type=MESH)

    def rs_right(i):
        zs = i
        return pltpu.make_async_remote_copy(
            src_ref=dxs.at[3, zs], dst_ref=left_in.at[zs], send_sem=out_s.at[1, i], recv_sem=left_r.at[i],
            device_id=(me, right), device_id_type=MESH)

    def stage_c(i):
        zs = i
        for kind in (1, 2, 4, 5):
            gat_in(kind, i).wait_recv()
        acc_g[...] = jnp.zeros_like(acc_g)
        acc_u[...] = jnp.zeros_like(acc_u)
        acc_d[...] = jnp.zeros_like(acc_d)

        def forward(q, c):
            xq = xb[q, zs, :, 0:F]
            acc_g[...] += dot_lanes(xq, wq[0, q, :, 0:F])
            acc_u[...] += dot_lanes(xq, wq[1, q, :, 0:F])
            acc_d[...] += dot_lanes(db[q, zs, :, 0:F], wq[2, q, :, 0:F])
            return c

        lax.fori_loop(0, NT, forward, 0)

        def elementwise(r, c):
            rows = pl.ds(pl.multiple_of(r * 16, 16), 16)
            gate, up, back = acc_g[rows, :], acc_u[rows, :] + 1.0, acc_d[rows, :]
            p = xb[t, zs, rows, F : F + 1].astype(F32)
            sig = 1.0 / (1.0 + jnp.exp(-SLOPE * gate))
            swish = gate * sig
            active = (swish * up).astype(BF16).astype(F32)
            prob[rows, :] = jnp.broadcast_to(jnp.sum(active * back, axis=1, keepdims=True), (16, 128))
            delta = p * back
            pa[zs, rows, 0:F] = (p * active).astype(BF16)
            dg[zs, rows, 0:F] = (delta * up * (sig + SLOPE * swish * (1.0 - sig))).astype(BF16)
            du[zs, rows, 0:F] = (delta * swish).astype(BF16)
            return c

        lax.fori_loop(0, GR // 16, elementwise, 0)

        def backward(r, c):
            q = (t + 2 + r) % NT
            part = dot(dg[zs, :, 0:F], wq[0, q, :, 0:F]) + dot(du[zs, :, 0:F], wq[1, q, :, 0:F])
            dxs[r, zs, :, 0:F] = part.astype(BF16)
            dxs[r, zs, :, F:FP] = prob[:, 0 : FP - F].astype(BF16)
            return c

        lax.fori_loop(0, NT, backward, 0)
        rs_far(i).start()
        if i % 2 == 0:
            rs_right(i).start()
        else:
            rs_left(i).start()

    def stage_s(i):
        zs = i
        rs_far(i).wait()
        role = 1 if i % 2 == 0 else 3
        dxs[role, zs] = (dxs[role, zs].astype(F32) + far_in[zs].astype(F32)).astype(BF16)
        if i % 2 == 0:
            rs_left(i).start()
        else:
            rs_right(i).start()

    def back(i, j):
        return pltpu.make_async_remote_copy(
            src_ref=ret.at[i * PL + j], dst_ref=ret_in.at[i * PL + j // 2 * 2 + core],
            send_sem=ret_s.at[i * PL + j], recv_sem=ret_r.at[i * PL + j // 2 * 2 + core],
            device_id=(source(i, j), t), device_id_type=MESH)

    def back_in(i, j):
        return pltpu.make_async_remote_copy(
            src_ref=ret.at[i * PL + j], dst_ref=ret_in.at[i * PL + j],
            send_sem=ret_s.at[i * PL + j], recv_sem=ret_r.at[i * PL + j],
            device_id=(dest(i, j), t), device_id_type=MESH)

    def stage_e(i):
        zs = i
        rs_left(i).wait()
        rs_right(i).wait()
        total = dxs[2, zs].astype(F32) + left_in[zs].astype(F32) + right_in[zs].astype(F32)
        rows = dot(rx_ref[...], total.astype(BF16))
        for j in range(PL):
            ret[i * PL + j] = rows[j * RB : (j + 1) * RB].astype(BF16)
        if i == 0:

            def keep(j):
                ret_in[j] = ret[j]

            own(keep)
        others(i, lambda j: back(i, j).start())

    def turn(w):
        turned[w] = fac[w].reshape(G * GR, FP)[:, 0:F].T

    def grad(w, quarters):
        for q in quarters:
            rows = xd[w // 2, q].reshape(G * GR, FP)[:, 0:F]
            grads[w, :, q * F : (q + 1) * F] = dot(turned[w], rows).astype(BF16)

    stage_b(0)
    stage_b(1)
    stage_b(2)
    stage_d(0)
    stage_b(3)
    stage_d(1)
    cut(0)
    stage_f(0)
    stage_d(2)
    stage_f(1)
    cut(1)
    stage_d(3)
    cut(2)
    stage_c(0)
    stage_f(2)
    stage_c(1)
    stage_f(3)
    stage_s(0)
    stage_c(2)
    stage_s(1)
    stage_c(3)
    stage_e(0)
    stage_s(2)
    stage_e(1)
    turn(0)
    grad(0, (0,))
    grad(0, (1,))
    turn(1)
    stage_s(3)
    grad(0, (2,))
    grad(0, (3,))
    grad(1, (0,))
    stage_e(2)
    turn(2)
    grad(1, (1,))
    stage_e(3)
    grad(1, (2,))
    grad(1, (3,))
    grad(2, (0,))
    grad(2, (1,))
    grad(2, (2,))
    grad(2, (3,))

    for i in range(G):
        for kind in range(6):
            gat_out(kind, i).wait_send()

    for i in range(G):

        def finish(j):
            a2a(i, j).wait_send()
            back(i, j).wait_send()
            back_in(i, j).wait_recv()

        others(i, finish)
        for j in range(PL):
            back_out[dest(i, j)] = ret_in[i * PL + j]


def combine_kernel(
    ids_ref, prow_ref, c24_ref, back_ref, grads, in_grad, gate_grad, up_grad, down_grad, prob_grad, sem
):
    writes = [
        pltpu.make_async_copy(grads.at[w], dst, sem.at[w]) for w, dst in enumerate((gate_grad, up_grad, down_grad))
    ]
    for w in writes:
        w.start()
    ids = ids_ref[...]
    table = owner_table(prow_ref[...])
    ranks = route_ranks(ids, table)
    mine = iota((NDP * RB, 128), 1) == c24_ref[:, 0:1]
    slots = dot(jnp.where(mine, 1.0, 0.0).astype(BF16), ranks)
    hot = jnp.where(slots == c24_ref[:, 1:2].astype(F32), 1.0, 0.0).astype(BF16)
    in_grad[...] = dot(back_ref[:, 0:F].T, hot).astype(BF16)
    prob = jnp.where(mine, back_ref[:, FP - 128 :][:, 127:128].astype(F32), 0.0).astype(BF16)
    by_owner = dot(prob.T, hot)
    for k in range(4):
        owner = dot(table, jnp.where(picks(ids, k), 1.0, 0.0).astype(BF16))
        prob_grad[k : k + 1, :] = jnp.sum(owner * by_owner, axis=0, keepdims=True).astype(BF16)
    for w in writes:
        w.wait()


def tables():
    r = np.arange(PL * SB)
    jj, j = r % SB, r // SB
    columns = [np.where(jj < CAP, jj, -5), np.where((jj >= DOFF) & (jj < DOFF + CAP), jj - DOFF, -5)]
    for chips in NEAR:
        columns += [np.array(chips)[j // 2, 0], np.array(chips)[j // 2, 1], j % 2]
    c40 = np.stack(columns, axis=1).astype(np.int32)
    cx = np.zeros((GR, PL * SB), np.float32)
    cd = np.zeros((GR, PL * SB), np.float32)
    rx = np.zeros((PL * RB, GR), np.float32)
    for j in range(PL):
        for k in range(CAP):
            cx[j * CAP + k, j * SB + k] = 1
            cd[j * CAP + k, j * SB + DOFF + k] = 1
            rx[j * RB + k, j * CAP + k] = 1
    r = np.arange(NDP * RB)
    c24 = np.stack([r // RB, r % RB], axis=1).astype(np.int32)
    return c40, cx, cd, rx, c24


def shards(tokens, out_grad, route_probs, expert_ids, placement_map, w_gate, w_up, w_down):
    c40, cx, cd, rx, c24 = tables()
    ids, prow = expert_ids.T, placement_map[None, :]
    vmem = pl.BlockSpec(memory_space=pltpu.VMEM)
    hbm = pl.BlockSpec(memory_space=pl.ANY)
    turned = jax.ShapeDtypeStruct((F, G * GR), BF16)
    dma = pltpu.SemaphoreType.DMA
    grads, back = pl.pallas_call(
        comm_kernel,
        out_shape=(pltpu.VMEM((3, F, NT * F), BF16), pltpu.VMEM((NDP, RB, FP), BF16)),
        in_specs=[vmem] * 9 + [hbm] * 3,
        out_specs=[vmem, vmem],
        scratch_shapes=[
            pltpu.VMEM((NDP, SB, FP), BF16), pltpu.VMEM((NDP, SB, FP), BF16),
            pltpu.VMEM((2, NT, G, GR, FP), BF16),
            pltpu.VMEM((3, WR, NT * F), BF16), pltpu.VMEM((3, NT, F, FP), BF16),
            pltpu.VMEM((GR, F), F32), pltpu.VMEM((GR, F), F32), pltpu.VMEM((GR, F), F32),
            pltpu.VMEM((3, G, GR, FP), BF16),
            pltpu.VMEM((GR, 128), F32),
            pltpu.VMEM((NT, G, GR, FP), BF16),
            pltpu.VMEM((G, GR, FP), BF16), pltpu.VMEM((G, GR, FP), BF16), pltpu.VMEM((G, GR, FP), BF16),
            pltpu.VMEM((NDP, RB, FP), BF16), pltpu.VMEM((NDP, RB, FP), BF16),
            pltpu.VMEM((3, F, G * GR), BF16),
            dma((3,)), dma((NDP,)), dma((NDP,)), dma((6, G)), dma((6, G)), dma((G,)), dma((G,)),
            dma((2, G)), dma((G,)), dma((G,)), dma((NDP,)), dma((NDP,)),
        ],
        compiler_params=pltpu.CompilerParams(
            collective_id=0, has_side_effects=True, vmem_limit_bytes=EXCHANGE_VMEM
        ),
        name="exchange",
    )(
        ids, prow, route_probs.T, tokens.T, out_grad.T,
        jnp.asarray(c40), jnp.asarray(cx, BF16), jnp.asarray(cd, BF16), jnp.asarray(rx, BF16),
        w_gate[0].T, w_up[0].T, w_down[0],
    )
    grad = jax.ShapeDtypeStruct((F, NT * F), BF16)
    in_grad, gate_grad, up_grad, down_grad, prob_grad = pl.pallas_call(
        combine_kernel,
        out_shape=(
            jax.ShapeDtypeStruct((F, TOK), BF16), grad, grad, grad, jax.ShapeDtypeStruct((4, TOK), BF16),
        ),
        in_specs=[vmem] * 5,
        out_specs=[vmem, hbm, hbm, hbm, vmem],
        scratch_shapes=[dma((3,))],
        compiler_params=pltpu.CompilerParams(vmem_limit_bytes=COMBINE_VMEM),
        name="combine",
    )(ids, prow, jnp.asarray(c24), back.reshape(NDP * RB, FP), grads)
    return (in_grad.T, gate_grad.T[None], up_grad.T[None], down_grad[None], prob_grad.T)


def solution(mesh):
    in_specs = (
        P("dp", "tensor"), P("dp", "tensor"), P("dp", None), P("dp", None), P(),
        P("dp", None, "tensor"), P("dp", None, "tensor"), P("dp", "tensor", None),
    )
    out_specs = (
        P("dp", "tensor"), P("dp", None, "tensor"), P("dp", None, "tensor"),
        P("dp", "tensor", None), P("dp", None),
    )
    return jax.shard_map(shards, mesh=mesh, in_specs=in_specs, out_specs=out_specs, check_vma=False)
```

```python
import functools

import jax
import jax.numpy as jnp
import numpy as np
from jax import lax
from jax.experimental import pallas as pl
from jax.experimental.pallas import tpu as pltpu
from jax.sharding import PartitionSpec as P

SLOPE = 1.702
MESH = pl.DeviceIdType.MESH
NDP, NT = 32, 4
CAP = 18
TOK, F, FP = 384, 720, 768
SB, DOFF = 40, 20
RB = 24
PL = 8
G = 4
GR = PL * CAP
WR, WCH = 144, 5
EXCHANGE_VMEM, COMBINE_VMEM = 48 * 2**20, 16 * 2**20
SRC_ORDER = (0, 1, 2, 3)
DST_ORDER = (0, 3, 2, 1)
LANES = (((1,), (1,)), ((), ()))
F32, BF16 = jnp.float32, jnp.bfloat16


def dot(a, b):
    return jnp.dot(a, b, preferred_element_type=F32)


def dot_lanes(a, b):
    return lax.dot_general(a, b, LANES, preferred_element_type=F32)


def iota(shape, dim):
    return lax.broadcasted_iota(jnp.int32, shape, dim)


def owner_table(prow):
    return jnp.where(prow == 4 * iota((128, 128), 0), 1.0, 0.0).astype(BF16)


def picks(ids, k):
    return iota((128, TOK), 0) == ids[k : k + 1, :]


def route_ranks(ids, table):
    hit = jnp.zeros((128, TOK), F32)
    for k in range(4):
        hit += jnp.where(picks(ids, k), 1.0, 0.0)
    member = dot(table, hit.astype(BF16))
    earlier = jnp.where(iota((TOK, TOK), 0) < iota((TOK, TOK), 1), 1.0, 0.0).astype(BF16)
    rank = dot(member.astype(BF16), earlier)
    return jnp.where(member > 0.5, rank, -1.0).astype(BF16)


def comm_kernel(
    ids_ref, prow_ref, probs_ref, tok_ref, og_ref, c40_ref, cx_ref, cd_ref, rx_ref, wg_hbm, wu_hbm, wd_hbm,
    grads, back_out,
    send, recv, xd, stage, wq, acc_g, acc_u, acc_d, fac, prob, dxs, far_in, left_in, right_in, ret, ret_in, turned,
    w_sem, a2a_s, a2a_r, gat_s, gat_r, far_s, far_r, out_s, left_r, right_r, ret_s, ret_r,
):
    me = lax.axis_index("dp")
    t = lax.axis_index("tensor")
    z = me // PL
    right, left, far = (t + 1) % NT, (t + 3) % NT, (t + 2) % NT

    xb, db = xd.at[0], xd.at[1]
    dg, du, pa = fac.at[0], fac.at[1], fac.at[2]

    barrier = pltpu.get_barrier_semaphore()

    def greet(d, c):
        @pl.when(d != me)
        def _():
            pl.semaphore_signal(barrier, inc=1, device_id=(d, t), device_id_type=MESH)

        return c

    lax.fori_loop(0, NDP, greet, 0)
    for nb in (left, right):
        pl.semaphore_signal(barrier, inc=1, device_id=(me, nb), device_id_type=MESH)

    weights = (wg_hbm, wu_hbm, wd_hbm)

    def load(n):
        w, r = n // WCH, n % WCH
        return pltpu.make_async_copy(
            weights[w].at[r * WR : (r + 1) * WR], stage.at[n % 3], w_sem.at[n % 3])

    for n in range(3):
        load(n).start()

    ids = ids_ref[...]
    table = owner_table(prow_ref[...])
    probs = probs_ref[...].astype(F32)
    ranks = route_ranks(ids, table)
    pw = jnp.zeros((128, TOK), F32)
    for k in range(4):
        pw += jnp.where(picks(ids, k), probs[k : k + 1, :], 0.0)
    owner_p = dot(table, pw.astype(BF16)).astype(BF16)

    def plane(order, i):
        return (z + order[i]) % G

    def build(zd):
        block, jx, jd = c40_ref[:, 0:1], c40_ref[:, 1:2], c40_ref[:, 2:3]
        mine = iota((PL * SB, 128), 1) == block + zd * PL
        slots = dot(jnp.where(mine, 1.0, 0.0).astype(BF16), ranks)
        hot_x = jnp.where(slots == jx.astype(F32), 1.0, 0.0).astype(BF16)
        hot_d = jnp.where(slots == jd.astype(F32), 1.0, 0.0).astype(BF16)
        rows = dot_lanes(hot_x, tok_ref[...]) + dot_lanes(hot_d, og_ref[...])
        p = jnp.sum(jnp.where(mine, dot_lanes(hot_x, owner_p), 0.0), axis=1, keepdims=True)
        for j in range(PL):
            part = slice(j * SB, (j + 1) * SB)
            send[zd * PL + j, :, 0:F] = rows[part].astype(BF16)
            send[zd * PL + j, :, F:FP] = jnp.broadcast_to(p[part], (SB, FP - F)).astype(BF16)

    def a2a(o):
        return pltpu.make_async_remote_copy(
            src_ref=send.at[o], dst_ref=recv.at[me], send_sem=a2a_s.at[o], recv_sem=a2a_r.at[me],
            device_id=(o, t), device_id_type=MESH)

    def a2a_in(s):
        return pltpu.make_async_remote_copy(
            src_ref=send.at[s], dst_ref=recv.at[s], send_sem=a2a_s.at[s], recv_sem=a2a_r.at[s],
            device_id=(s, t), device_id_type=MESH)

    def others(first, act):
        def body(j, c):
            o = first + j

            @pl.when(o != me)
            def _():
                act(o)

            return c

        lax.fori_loop(0, PL, body, 0)

    def stage_b(i):
        zd = plane(DST_ORDER, i)
        build(zd)
        if i == 0:
            pl.semaphore_wait(barrier, NDP - 1 + 2)
            recv[me] = send[me]
        others(zd * PL, lambda o: a2a(o).start())

    def cut(w):
        for r in range(WCH):
            n = w * WCH + r
            load(n).wait()
            for q in range(NT):
                wq[w, q, r * WR : (r + 1) * WR, 0:F] = stage[n % 3, :, q * F : (q + 1) * F]
            if n + 3 < 3 * WCH:
                load(n + 3).start()

    def gat(kind, i, ref, q, to):
        zs = plane(SRC_ORDER, i)
        return pltpu.make_async_remote_copy(
            src_ref=ref.at[q, zs], dst_ref=ref.at[q, zs], send_sem=gat_s.at[kind, i], recv_sem=gat_r.at[kind, i],
            device_id=(me, to), device_id_type=MESH)

    def gat_out(kind, i):
        return (
            lambda: gat(0, i, xb, t, right), lambda: gat(1, i, xb, t, left),
            lambda: gat(2, i, db, t, right), lambda: gat(3, i, db, t, left),
            lambda: gat(4, i, xb, left, right), lambda: gat(5, i, db, right, left),
        )[kind]()

    def gat_in(kind, i):
        return (
            lambda: gat(0, i, xb, left, right), lambda: gat(1, i, xb, right, left),
            lambda: gat(2, i, db, left, right), lambda: gat(3, i, db, right, left),
            lambda: gat(4, i, xb, far, right), lambda: gat(5, i, db, far, left),
        )[kind]()

    def stage_d(i):
        zs = plane(SRC_ORDER, i)
        others(zs * PL, lambda s: a2a_in(s).wait_recv())
        got = recv[pl.ds(zs * PL, PL)].reshape(PL * SB, FP)
        xb[t, zs] = dot(cx_ref[...], got).astype(BF16)
        db[t, zs] = dot(cd_ref[...], got).astype(BF16)
        for kind in range(4):
            gat_out(kind, i).start()

    def stage_f(i):
        gat_in(0, i).wait_recv()
        gat_out(4, i).start()
        gat_in(3, i).wait_recv()
        gat_out(5, i).start()

    def rs_far(i):
        zs = plane(SRC_ORDER, i)
        return pltpu.make_async_remote_copy(
            src_ref=dxs.at[0, zs], dst_ref=far_in.at[zs], send_sem=far_s.at[i], recv_sem=far_r.at[i],
            device_id=(me, left if i % 2 == 0 else right), device_id_type=MESH)

    def rs_left(i):
        zs = plane(SRC_ORDER, i)
        return pltpu.make_async_remote_copy(
            src_ref=dxs.at[1, zs], dst_ref=right_in.at[zs], send_sem=out_s.at[0, i], recv_sem=right_r.at[i],
            device_id=(me, left), device_id_type=MESH)

    def rs_right(i):
        zs = plane(SRC_ORDER, i)
        return pltpu.make_async_remote_copy(
            src_ref=dxs.at[3, zs], dst_ref=left_in.at[zs], send_sem=out_s.at[1, i], recv_sem=left_r.at[i],
            device_id=(me, right), device_id_type=MESH)

    def stage_c(i):
        zs = plane(SRC_ORDER, i)
        for kind in (1, 2, 4, 5):
            gat_in(kind, i).wait_recv()
        acc_g[...] = jnp.zeros_like(acc_g)
        acc_u[...] = jnp.zeros_like(acc_u)
        acc_d[...] = jnp.zeros_like(acc_d)

        def forward(q, c):
            xq = xb[q, zs, :, 0:F]
            acc_g[...] += dot_lanes(xq, wq[0, q, :, 0:F])
            acc_u[...] += dot_lanes(xq, wq[1, q, :, 0:F])
            acc_d[...] += dot_lanes(db[q, zs, :, 0:F], wq[2, q, :, 0:F])
            return c

        lax.fori_loop(0, NT, forward, 0)

        def elementwise(r, c):
            rows = pl.ds(pl.multiple_of(r * 16, 16), 16)
            gate, up, back = acc_g[rows, :], acc_u[rows, :] + 1.0, acc_d[rows, :]
            p = xb[t, zs, rows, F : F + 1].astype(F32)
            sig = 1.0 / (1.0 + jnp.exp(-SLOPE * gate))
            swish = gate * sig
            active = (swish * up).astype(BF16).astype(F32)
            prob[rows, :] = jnp.broadcast_to(jnp.sum(active * back, axis=1, keepdims=True), (16, 128))
            delta = p * back
            pa[zs, rows, 0:F] = (p * active).astype(BF16)
            dg[zs, rows, 0:F] = (delta * up * (sig + SLOPE * swish * (1.0 - sig))).astype(BF16)
            du[zs, rows, 0:F] = (delta * swish).astype(BF16)
            return c

        lax.fori_loop(0, GR // 16, elementwise, 0)

        def backward(r, c):
            q = (t + 2 + r) % NT
            part = dot(dg[zs, :, 0:F], wq[0, q, :, 0:F]) + dot(du[zs, :, 0:F], wq[1, q, :, 0:F])
            dxs[r, zs, :, 0:F] = part.astype(BF16)
            dxs[r, zs, :, F:FP] = prob[:, 0 : FP - F].astype(BF16)
            return c

        backward(0, 0)
        rs_far(i).start()
        lax.fori_loop(1, NT, backward, 0)
        if i % 2 == 0:
            rs_right(i).start()
        else:
            rs_left(i).start()

    def stage_s(i):
        zs = plane(SRC_ORDER, i)
        rs_far(i).wait()
        role = 1 if i % 2 == 0 else 3
        dxs[role, zs] = (dxs[role, zs].astype(F32) + far_in[zs].astype(F32)).astype(BF16)
        if i % 2 == 0:
            rs_left(i).start()
        else:
            rs_right(i).start()

    def back(s):
        return pltpu.make_async_remote_copy(
            src_ref=ret.at[s], dst_ref=ret_in.at[me], send_sem=ret_s.at[s], recv_sem=ret_r.at[me],
            device_id=(s, t), device_id_type=MESH)

    def back_in(o):
        return pltpu.make_async_remote_copy(
            src_ref=ret.at[o], dst_ref=ret_in.at[o], send_sem=ret_s.at[o], recv_sem=ret_r.at[o],
            device_id=(o, t), device_id_type=MESH)

    def stage_e(i):
        zs = plane(SRC_ORDER, i)
        rs_left(i).wait()
        rs_right(i).wait()
        total = dxs[2, zs].astype(F32) + left_in[zs].astype(F32) + right_in[zs].astype(F32)
        rows = dot(rx_ref[...], total.astype(BF16))
        for j in range(PL):
            ret[zs * PL + j] = rows[j * RB : (j + 1) * RB].astype(BF16)
        if i == 0:
            ret_in[me] = ret[me]
        others(zs * PL, lambda s: back(s).start())

    def turn(w):
        turned[w] = fac[w].reshape(G * GR, FP)[:, 0:F].T

    def grad(w, quarters):
        for q in quarters:
            rows = xd[w // 2, q].reshape(G * GR, FP)[:, 0:F]
            grads[w, :, q * F : (q + 1) * F] = dot(turned[w], rows).astype(BF16)

    stage_b(0)
    stage_b(1)
    stage_b(2)
    stage_d(0)
    stage_b(3)
    stage_d(1)
    cut(0)
    stage_f(0)
    cut(1)
    stage_f(1)
    stage_d(2)
    cut(2)
    stage_d(3)
    stage_c(0)
    stage_f(2)
    stage_c(1)
    stage_f(3)
    stage_s(0)
    stage_c(2)
    stage_s(1)
    stage_c(3)
    stage_e(0)
    stage_s(2)
    stage_e(1)
    turn(0)
    grad(0, (0,))
    grad(0, (1,))
    turn(1)
    stage_s(3)
    grad(0, (2,))
    grad(0, (3,))
    grad(1, (0,))
    stage_e(2)
    turn(2)
    grad(1, (1,))
    stage_e(3)
    grad(1, (2,))
    grad(1, (3,))
    grad(2, (0,))
    grad(2, (1,))
    grad(2, (2,))
    grad(2, (3,))

    for i in range(G):
        for kind in range(6):
            gat_out(kind, i).wait_send()

    def finish(o, c):
        @pl.when(o != me)
        def _():
            a2a(o).wait_send()
            back(o).wait_send()
            back_in(o).wait_recv()

        return c

    lax.fori_loop(0, NDP, finish, 0)

    def hand_on(o, c):
        back_out[o] = ret_in[o]
        return c

    lax.fori_loop(0, NDP, hand_on, 0)


def combine_kernel(
    ids_ref, prow_ref, c24_ref, back_ref, grads, in_grad, gate_grad, up_grad, down_grad, prob_grad, sem
):
    writes = [
        pltpu.make_async_copy(grads.at[w], dst, sem.at[w]) for w, dst in enumerate((gate_grad, up_grad, down_grad))
    ]
    for w in writes:
        w.start()
    ids = ids_ref[...]
    table = owner_table(prow_ref[...])
    ranks = route_ranks(ids, table)
    mine = iota((NDP * RB, 128), 1) == c24_ref[:, 0:1]
    slots = dot(jnp.where(mine, 1.0, 0.0).astype(BF16), ranks)
    hot = jnp.where(slots == c24_ref[:, 1:2].astype(F32), 1.0, 0.0).astype(BF16)
    in_grad[...] = dot(back_ref[:, 0:F].T, hot).astype(BF16)
    prob = jnp.where(mine, back_ref[:, FP - 128 :][:, 127:128].astype(F32), 0.0).astype(BF16)
    by_owner = dot(prob.T, hot)
    for k in range(4):
        owner = dot(table, jnp.where(picks(ids, k), 1.0, 0.0).astype(BF16))
        prob_grad[k : k + 1, :] = jnp.sum(owner * by_owner, axis=0, keepdims=True).astype(BF16)
    for w in writes:
        w.wait()


def tables():
    r = np.arange(PL * SB)
    jj = r % SB
    jx = np.where(jj < CAP, jj, -5)
    jd = np.where((jj >= DOFF) & (jj < DOFF + CAP), jj - DOFF, -5)
    c40 = np.stack([r // SB, jx, jd], axis=1).astype(np.int32)
    cx = np.zeros((GR, PL * SB), np.float32)
    cd = np.zeros((GR, PL * SB), np.float32)
    rx = np.zeros((PL * RB, GR), np.float32)
    for j in range(PL):
        for k in range(CAP):
            cx[j * CAP + k, j * SB + k] = 1
            cd[j * CAP + k, j * SB + DOFF + k] = 1
            rx[j * RB + k, j * CAP + k] = 1
    r = np.arange(NDP * RB)
    c24 = np.stack([r // RB, r % RB], axis=1).astype(np.int32)
    return c40, cx, cd, rx, c24


def shards(tokens, out_grad, route_probs, expert_ids, placement_map, w_gate, w_up, w_down):
    c40, cx, cd, rx, c24 = tables()
    ids, prow = expert_ids.T, placement_map[None, :]
    vmem = pl.BlockSpec(memory_space=pltpu.VMEM)
    hbm = pl.BlockSpec(memory_space=pl.ANY)
    turned = jax.ShapeDtypeStruct((F, G * GR), BF16)
    dma = pltpu.SemaphoreType.DMA
    grads, back = pl.pallas_call(
        comm_kernel,
        out_shape=(pltpu.VMEM((3, F, NT * F), BF16), pltpu.VMEM((NDP, RB, FP), BF16)),
        in_specs=[vmem] * 9 + [hbm] * 3,
        out_specs=[vmem, vmem],
        scratch_shapes=[
            pltpu.VMEM((NDP, SB, FP), BF16), pltpu.VMEM((NDP, SB, FP), BF16),
            pltpu.VMEM((2, NT, G, GR, FP), BF16),
            pltpu.VMEM((3, WR, NT * F), BF16), pltpu.VMEM((3, NT, F, FP), BF16),
            pltpu.VMEM((GR, F), F32), pltpu.VMEM((GR, F), F32), pltpu.VMEM((GR, F), F32),
            pltpu.VMEM((3, G, GR, FP), BF16),
            pltpu.VMEM((GR, 128), F32),
            pltpu.VMEM((NT, G, GR, FP), BF16),
            pltpu.VMEM((G, GR, FP), BF16), pltpu.VMEM((G, GR, FP), BF16), pltpu.VMEM((G, GR, FP), BF16),
            pltpu.VMEM((NDP, RB, FP), BF16), pltpu.VMEM((NDP, RB, FP), BF16),
            pltpu.VMEM((3, F, G * GR), BF16),
            dma((3,)), dma((NDP,)), dma((NDP,)), dma((6, G)), dma((6, G)), dma((G,)), dma((G,)),
            dma((2, G)), dma((G,)), dma((G,)), dma((NDP,)), dma((NDP,)),
        ],
        compiler_params=pltpu.CompilerParams(
            collective_id=0, has_side_effects=True, vmem_limit_bytes=EXCHANGE_VMEM
        ),
        name="exchange",
    )(
        ids, prow, route_probs.T, tokens.T, out_grad.T,
        jnp.asarray(c40), jnp.asarray(cx, BF16), jnp.asarray(cd, BF16), jnp.asarray(rx, BF16),
        w_gate[0].T, w_up[0].T, w_down[0],
    )
    grad = jax.ShapeDtypeStruct((F, NT * F), BF16)
    in_grad, gate_grad, up_grad, down_grad, prob_grad = pl.pallas_call(
        combine_kernel,
        out_shape=(
            jax.ShapeDtypeStruct((F, TOK), BF16), grad, grad, grad, jax.ShapeDtypeStruct((4, TOK), BF16),
        ),
        in_specs=[vmem] * 5,
        out_specs=[vmem, hbm, hbm, hbm, vmem],
        scratch_shapes=[dma((3,))],
        compiler_params=pltpu.CompilerParams(vmem_limit_bytes=COMBINE_VMEM),
        name="combine",
    )(ids, prow, jnp.asarray(c24), back.reshape(NDP * RB, FP), grads)
    return (in_grad.T, gate_grad.T[None], up_grad.T[None], down_grad[None], prob_grad.T)


def solution(mesh):
    in_specs = (
        P("dp", "tensor"), P("dp", "tensor"), P("dp", None), P("dp", None), P(),
        P("dp", None, "tensor"), P("dp", None, "tensor"), P("dp", "tensor", None),
    )
    out_specs = (
        P("dp", "tensor"), P("dp", None, "tensor"), P("dp", None, "tensor"),
        P("dp", "tensor", None), P("dp", None),
    )
    return jax.shard_map(shards, mesh=mesh, in_specs=in_specs, out_specs=out_specs, check_vma=False)
```
